128 devices in a mesh: dp: 16 (over y, x_lo, core), tensor: 8 (over z, x_hi).
Axes of the slice: x: 4 (x_hi: 2, x_lo: 2; x = x_hi * 2 + x_lo), y: 4, z: 4, core: 2. Of those that a mesh axis runs over, the one named last changes fastest.
Arguments:
- arrived: bfloat16 [256, 128, 1536], P(('dp', 'tensor')), may hold values from -6 to 6
- destination: int32 [256], replicated, may hold values from 0 to 15, as said below
- query_of: int32 [256], replicated, may hold values from 0 to 31, as said below
- lengths: int32 [256], replicated, may hold values from 32 to 128
- attn_gain: float32 [1536], replicated, may hold values from 0.25 to 1.75
- q_weight: bfloat16 [1536, 1024], P(None, 'tensor')
- q_bias: bfloat16 [1024], P('tensor'), may hold values from -3 to 3
- k_weight: bfloat16 [1536, 256], replicated
- v_weight: bfloat16 [1536, 256], replicated, may hold values from -0.15625 to 0.15625
- v_bias: bfloat16 [256], replicated, may hold values from -3 to 3
- o_weight: bfloat16 [1024, 1536], P('tensor'), may hold values from -0.1875 to 0.1875
- mlp_gain: float32 [1536], replicated, may hold values from 0.25 to 1.75
- w_gate: bfloat16 [1536, 8960], P(None, 'tensor'), may hold values from -0.15625 to 0.15625
- w_up: bfloat16 [1536, 8960], P(None, 'tensor'), may hold values from -0.15625 to 0.15625
- w_down: bfloat16 [8960, 1536], P('tensor'), may hold values from -0.0625 to 0.0625
- final_gain: float32 [1536], replicated, may hold values from 0.25 to 1.75
- score_weight: float32 [1536], replicated, may hold values from -0.15625 to 0.15625
Outputs:
- hidden_out: bfloat16 [128, 256, 1536], P('tensor', 'dp')
- centred: float32 [256], P('dp')
- query_mean: float32 [32], P('dp')
The draws below stay inside these ranges and needn't reach their ends.
Inputs may be any that keep to these rules, and one draw needn't show every extreme that they name: In each aligned block of 16 pairs every destination occurs exactly once. `query_of`: each query has exactly 8 pairs.
All inputs are finite; a program needn't handle non-finite values.
Results may differ from the reference program's by a relative error of at most 0.02.
The reference program's roundings to bfloat16 on the way (of `relaid`, `normed`, `probs`, `context`, `after_attention`, `normed_mlp` and `activated`) count: a program that leaves them out, or rounds other values in their place, can miss the bound.
Values may be sent and summed in bfloat16 or wider, within the bound.
A program may use at most 128 MiB of HBM per device.

```python
import math
import jax
import jax.numpy as jnp
from jax import lax

D = 1536
FF = 8960
KV_HEADS = 2
HEAD_DIM = 128
HEADS = 8
SEQ = 128
PAIRS_DP = 16
PAIRS = 256
QUERIES = 32
N_TENSOR = 8


def draw_q_weight(key, part):
    drawn_part = jax.random.normal(jax.random.fold_in(key, 11), (D, HEADS * HEAD_DIM), jnp.float32) / math.sqrt(D)
    return drawn_part.astype(jnp.bfloat16)


def draw_k_weight(key, part):
    drawn_part = jax.random.normal(jax.random.fold_in(key, 13), (D, KV_HEADS * HEAD_DIM), jnp.float32) / math.sqrt(D)
    return drawn_part.astype(jnp.bfloat16)


def draw_destination(key, part):
    blocks = PAIRS // PAIRS_DP
    base_groups = jnp.arange(PAIRS_DP, dtype=jnp.int32) % blocks
    block_keys = jax.random.split(jax.random.fold_in(key, 21), blocks)
    shuffled = jax.vmap(lambda block_key: jax.random.permutation(block_key, base_groups))(block_keys)
    return shuffled.reshape(PAIRS).astype(jnp.int32)


def draw_query_of(key, part):
    shuffled = jax.random.permutation(jax.random.fold_in(key, 31), PAIRS)
    return (shuffled % QUERIES).astype(jnp.int32)


def touch_ends(values, rng, least, largest):
    shape = values.shape
    index_at = [jax.random.randint(jax.random.fold_in(rng, axis), (), 0, shape[axis]) for axis in range(len(shape))]
    values = values.at[tuple(index_at)].set(least)
    longest = shape.index(max(shape))
    index_at[longest] = (index_at[longest] + 1) % shape[longest]
    return values.at[tuple(index_at)].set(largest)


def steps_of(rng, extent, shards, least, top_value):
    factor_of, own = 1.0, jax.random.fold_in(rng, 6)
    for dim, parts in shards:
        heights = jnp.exp(jax.random.uniform(jax.random.fold_in(own, dim), (parts,), jnp.float32, least / len(shards), top_value / len(shards)))
        factor_of = factor_of * jnp.repeat(heights, extent[dim] // parts).reshape([-1 if axis == dim else 1 for axis in range(len(extent))])
    return factor_of


def noise(key, extent, spread, limit, shards=(), kind=jnp.bfloat16):
    level = steps_of(key, extent, shards, -0.22, 0.18) if shards else 1.0
    entries = jax.random.normal(key, extent, jnp.float32) * spread * level
    return jnp.minimum(jnp.maximum(entries, -limit), limit).astype(kind)


def setup_inputs(seed: int = 0) -> dict:
    keys = jax.random.split(jax.random.key(seed), 18)
    return {
        "arrived": noise(keys[0], (PAIRS, SEQ, D), 1.0, 6.0, ((0, 128),)),
        "destination": draw_destination(jax.random.fold_in(keys[17], 71), 0),
        "query_of": draw_query_of(jax.random.fold_in(keys[17], 71), 0),
        "lengths": touch_ends(jax.random.randint(keys[3], (PAIRS,), SEQ // 4, SEQ + 1), jax.random.fold_in(keys[3], 1), SEQ // 4, SEQ).astype(jnp.int32),
        "attn_gain": jnp.clip(1.0 + 0.15 * jax.random.normal(keys[4], (D,), jnp.float32), 0.25, 1.75),
        "q_weight": draw_q_weight(jax.random.fold_in(keys[17], 71), 0),
        "q_bias": noise(keys[6], (HEADS * HEAD_DIM,), 0.5, 3.0, ((0, 8),)),
        "k_weight": draw_k_weight(jax.random.fold_in(keys[17], 71), 0),
        "v_weight": noise(keys[8], (D, KV_HEADS * HEAD_DIM), D ** -0.5, 0.15625),
        "v_bias": noise(keys[9], (KV_HEADS * HEAD_DIM,), 0.5, 3.0),
        "o_weight": noise(keys[10], (HEADS * HEAD_DIM, D), (HEADS * HEAD_DIM) ** -0.5, 0.1875, ((0, 8),)),
        "mlp_gain": jnp.clip(1.0 + 0.15 * jax.random.normal(keys[11], (D,), jnp.float32), 0.25, 1.75),
        "w_gate": noise(keys[12], (D, FF), D ** -0.5, 0.15625, ((1, 8),)),
        "w_up": noise(keys[13], (D, FF), D ** -0.5, 0.15625, ((1, 8),)),
        "w_down": noise(keys[14], (FF, D), FF ** -0.5, 0.0625, ((0, 8),)),
        "final_gain": jnp.clip(1.0 + 0.15 * jax.random.normal(keys[15], (D,), jnp.float32), 0.25, 1.75),
        "score_weight": noise(keys[16], (D,), D ** -0.5, 0.15625, (), jnp.float32),
    }


theta_base = 1000000.0
norm_eps = 1e-06

def widen(values):
    return lax.optimization_barrier(values).astype(jnp.float32)

def rms_scale(values, gain_vector):
    floats = values.astype(jnp.float32)
    return floats * lax.rsqrt(lax.optimization_barrier(jnp.mean(floats * floats, axis=-1, keepdims=True)) + norm_eps) * gain_vector.astype(jnp.float32)

def frequency_table(head_dim):
    return theta_base ** (-2.0 * jnp.arange(head_dim // 2, dtype=jnp.float32) / head_dim)

def rotate(values, cosine_table, sine_table):
    half_dim = values.shape[-1] // 2
    first_half = values[..., :half_dim]
    second_half = values[..., half_dim:]
    return jnp.concatenate([first_half * cosine_table - second_half * sine_table, second_half * cosine_table + first_half * sine_table], axis=-1)

def reference(arrived, destination, query_of, lengths, attn_gain, q_weight, q_bias, k_weight, v_weight, v_bias, o_weight, mlp_gain, w_gate, w_up, w_down, final_gain, score_weight):
    relaid_order = jnp.argsort(destination * PAIRS + jnp.arange(PAIRS, dtype=jnp.int32)).astype(jnp.int32)
    relaid = jnp.take(arrived, relaid_order, axis=0)
    relaid_lengths = jnp.take(lengths, relaid_order)
    relaid_queries = jnp.take(query_of, relaid_order)
    angles = jnp.arange(SEQ, dtype=jnp.float32)[:, None] * frequency_table(HEAD_DIM)[None, :]
    cosine_table = jnp.cos(angles)[None, :, None, :]
    sine_table = jnp.sin(angles)[None, :, None, :]
    group_size = HEADS // KV_HEADS
    positions = jnp.arange(SEQ, dtype=jnp.int32)
    causal = positions[None, :] <= positions[:, None]
    block_units = FF // N_TENSOR

    def one_group(inputs):
        hidden, pair_lengths = inputs
        count_pairs = hidden.shape[0]
        normed = widen(rms_scale(hidden, attn_gain).astype(jnp.bfloat16))
        query_rows = jnp.einsum('psd,de->pse', normed, widen(q_weight)) + widen(q_bias)
        query_rows = rotate(query_rows.reshape(count_pairs, SEQ, HEADS, HEAD_DIM), cosine_table, sine_table).astype(jnp.bfloat16)
        key_rows = jnp.einsum('psd,de->pse', normed, widen(k_weight)).reshape(count_pairs, SEQ, KV_HEADS, HEAD_DIM)
        key_rows = rotate(key_rows, cosine_table, sine_table).astype(jnp.bfloat16)
        value_rows = (jnp.einsum('psd,de->pse', normed, widen(v_weight)) + widen(v_bias)).astype(jnp.bfloat16)
        value_rows = value_rows.reshape(count_pairs, SEQ, KV_HEADS, HEAD_DIM)
        keys_wide = jnp.repeat(widen(key_rows), group_size, axis=2)
        values_wide = jnp.repeat(widen(value_rows), group_size, axis=2)
        logits = jnp.einsum('pqhe,pkhe->phqk', widen(query_rows), keys_wide) / math.sqrt(HEAD_DIM)
        allowed = causal[None, :, :] & (positions[None, None, :] < pair_lengths[:, None, None])
        logits = jnp.where(allowed[:, None, :, :], logits, -1e+30)
        shifted = jnp.exp(logits - lax.optimization_barrier(jnp.max(logits, axis=-1, keepdims=True)))
        probs = (shifted / lax.optimization_barrier(jnp.sum(shifted, axis=-1, keepdims=True))).astype(jnp.bfloat16)
        context = jnp.einsum('phqk,pkhe->pqhe', widen(probs), values_wide).astype(jnp.bfloat16)
        context = context.reshape(count_pairs, SEQ, HEADS * HEAD_DIM)
        attended = jnp.einsum('pse,ed->psd', widen(context), widen(o_weight))
        after_attention = (widen(hidden) + attended).astype(jnp.bfloat16)
        normed_mlp = widen(rms_scale(after_attention, mlp_gain).astype(jnp.bfloat16))
        gate_values = jnp.einsum('psd,df->psf', normed_mlp, widen(w_gate))
        up_values = jnp.einsum('psd,df->psf', normed_mlp, widen(w_up))
        activated = widen((jax.nn.silu(gate_values) * up_values).astype(jnp.bfloat16))
        down_wide = widen(w_down)
        mlp_sum = jnp.zeros((count_pairs, SEQ, D), jnp.float32)
        for block in range(N_TENSOR):
            partial_value = jnp.einsum('psf,fd->psd', activated[..., block * block_units:(block + 1) * block_units], down_wide[block * block_units:(block + 1) * block_units])
            mlp_sum = mlp_sum + widen(partial_value.astype(jnp.bfloat16))
        layer_out = (widen(after_attention) + mlp_sum).astype(jnp.bfloat16)
        last_rows = jnp.take_along_axis(layer_out, (pair_lengths - 1).astype(jnp.int32)[:, None, None], axis=1)[:, 0, :]
        pair_scores = lax.optimization_barrier(jnp.sum(rms_scale(last_rows, final_gain) * score_weight.astype(jnp.float32), axis=-1))
        return (layer_out, pair_scores)
    group_count = PAIRS // PAIRS_DP
    layer_outs, pair_scores = lax.map(one_group, (relaid.reshape(group_count, PAIRS_DP, SEQ, D), relaid_lengths.reshape(group_count, PAIRS_DP)))
    hidden_out = jnp.transpose(layer_outs.reshape(PAIRS, SEQ, D), (1, 0, 2))
    scores = pair_scores.reshape(PAIRS)
    membership = (relaid_queries[:, None] == jnp.arange(QUERIES, dtype=jnp.int32)[None, :]).astype(jnp.float32)
    totals = jnp.dot(scores, membership, precision=lax.Precision.HIGHEST)
    query_mean = totals / (PAIRS // QUERIES)
    centred = scores - jnp.dot(membership, query_mean, precision=lax.Precision.HIGHEST)
    return (hidden_out, centred, query_mean)
```

```python
import functools
import math

import jax
import jax.numpy as jnp
import numpy as np
from jax import lax
from jax.experimental import pallas as pl
from jax.experimental.pallas import tpu as pltpu
from jax.sharding import Mesh
from jax.sharding import PartitionSpec as P

AXES = ("y", "xl", "c", "z", "xh")
DP = ("y", "xl", "c")
TENSOR = ("z", "xh")
MESH = pl.DeviceIdType.MESH
F32 = jnp.float32
BF16 = jnp.bfloat16

KV_HEADS = 2
HEAD_DIM = 128
HEADS = 8
QUERY_DP = 2
theta_base = 1000000.0
norm_eps = 1e-06

SEQ = 128
D = 1536
FFL = 1120
FULL = 1024
TAIL = FFL - FULL
FFP = 1152

C1 = (0, 144)
C1A, C1B = (0, 80), (80, 144)
C2 = (144, 256)
C2A, C2B = (144, 208), (208, 256)
N1, N1A = 9, 5
N2A = 13


def z_at(step):
    return lax.rem(lax.axis_index("z") + step + 4, 4)


class Sender:
    def __init__(self, send_sem, recv_sem):
        self.send_sem, self.recv_sem, self.count = send_sem, recv_sem, 0
        self.open = []

    def __call__(self, src, dst, device):
        i = self.count
        self.count += 1
        copy = pltpu.make_async_remote_copy(
            src_ref=src,
            dst_ref=dst,
            send_sem=self.send_sem.at[i],
            recv_sem=self.recv_sem.at[i],
            device_id=device,
            device_id_type=MESH,
        )
        copy.start()
        self.open.append(copy)
        return copy

    def drain(self):
        for copy in self.open:
            copy.wait_send()
        self.open = []


def tensor_peer(k):
    index = lax.rem(lax.axis_index("z") * 2 + lax.axis_index("xh") + k, 8)
    return {"z": index // 2, "xh": lax.rem(index, 2)}


def dp_peer(k):
    index = lax.axis_index("y") * 4 + lax.axis_index("xl") * 2 + lax.axis_index("c")
    index = lax.rem(index + k, 16)
    return index, {"y": index // 4, "xl": lax.rem(index // 2, 2), "c": lax.rem(index, 2)}


def greet(devices):
    barrier = pltpu.get_barrier_semaphore()
    for device in devices:
        pl.semaphore_signal(barrier, inc=1, device_id=device, device_id_type=MESH)
    pl.semaphore_wait(barrier, len(devices))


def rms_rows(values, gain):
    scale = lax.rsqrt(jnp.mean(values * values, axis=-1, keepdims=True) + norm_eps)
    return values * scale * gain


def rotate(values, cosine, sine):
    return values * cosine + pltpu.roll(values, HEAD_DIM // 2, 1) * sine


def attention_kernel(
    lengths, gain, mlp_gain, q_bias, v_bias, cosine, sine, arrived, q_w, k_w, v_w, o_w,
    after_out, normed_out,
    x_v, k_v, v_v, q_all, o_all, bias_one, bias_all, normed, keys, values, queries, context,
    local_sem, send_sem, recv_sem,
):
    z, xh, c = lax.axis_index("z"), lax.axis_index("xh"), lax.axis_index("c")
    y, xl = lax.axis_index("y"), lax.axis_index("xl")
    t = z * 2 + xh
    partner, sibling = {"xh": 1 - xh}, {"c": 1 - c}
    up, down = {"z": z_at(1)}, {"z": z_at(-1)}

    def q_cols(index):
        return pl.ds(pl.multiple_of(index * HEAD_DIM, HEAD_DIM), HEAD_DIM)

    loads = [
        pltpu.make_async_copy(arrived, x_v, local_sem.at[0]),
        pltpu.make_async_copy(k_w, k_v, local_sem.at[1]),
        pltpu.make_async_copy(v_w, v_v, local_sem.at[2]),
        pltpu.make_async_copy(q_w, q_all.at[:, q_cols(t)], local_sem.at[3]),
        pltpu.make_async_copy(
            o_w, o_all.at[pl.ds(pl.multiple_of(t * HEAD_DIM, HEAD_DIM), HEAD_DIM)], local_sem.at[4]
        ),
    ]
    for load in loads:
        load.start()
    bias_one[...] = jnp.broadcast_to(q_bias[...].astype(F32), bias_one.shape)
    greet([tensor_peer(k) for k in range(1, 8)] + [sibling])
    send = Sender(send_sem, recv_sem)

    half_q, half_o = D // 2, HEAD_DIM // 2

    def q_piece(index, sub=None):
        size = half_q if sub is None else half_q // 2
        start = c * half_q + (0 if sub is None else sub * size)
        return q_all.at[pl.ds(pl.multiple_of(start, 128), size), q_cols(index)]

    def o_piece(index, sub=None):
        size = half_o if sub is None else half_o // 2
        start = index * HEAD_DIM + c * half_o + (0 if sub is None else sub * size)
        return o_all.at[pl.ds(pl.multiple_of(start, 32), size)]

    zp, zm, z2 = z_at(1), z_at(-1), z_at(2)
    own_q = q_w.at[pl.ds(pl.multiple_of(c * half_q, 128), half_q)]
    own_o = o_w.at[pl.ds(pl.multiple_of(c * half_o, 64), half_o)]

    def first(piece, own):
        return [send(own, piece(t), partner), send(own, piece(t), up), send(own, piece(t), down)]

    q_x, q_u, q_d = first(q_piece, own_q)
    bias_copies = [send(bias_one, bias_all.at[t], tensor_peer(k)) for k in range(1, 8)]
    o_x, o_u, o_d = first(o_piece, own_o)

    loads[0].wait()
    x = x_v[...].reshape(2 * SEQ, D)
    normed[...] = rms_rows(x.astype(F32), gain[...]).astype(BF16)
    loads[1].wait()
    loads[2].wait()
    cos_rows = jnp.concatenate([cosine[...]] * 2, axis=0)
    sin_rows = jnp.concatenate([sine[...]] * 2, axis=0)
    k_f = jnp.dot(normed[...], k_v[...], preferred_element_type=F32)
    for g in range(KV_HEADS):
        cols = slice(g * HEAD_DIM, (g + 1) * HEAD_DIM)
        keys[:, cols] = rotate(k_f[:, cols], cos_rows, sin_rows).astype(BF16)
    v_f = jnp.dot(normed[...], v_v[...], preferred_element_type=F32)
    values[...] = (v_f + v_bias[...].astype(F32)).astype(BF16)

    def second(piece, x_c, u_c, d_c):
        x_c.wait_recv()
        other = z * 2 + 1 - xh
        a = send(piece(other), piece(other), up)
        b = send(piece(other), piece(other), down)
        s = [send(piece(other), piece(other), sibling)]
        u_c.wait_recv()
        low, high = zm * 2 + xh, zp * 2 + xh
        f = send(piece(low, 0), piece(low, 0), up)
        s.append(send(piece(low), piece(low), sibling))
        d_c.wait_recv()
        h = send(piece(high, 1), piece(high, 1), down)
        s.append(send(piece(high), piece(high), sibling))
        return a, b, f, h, s

    def third(piece, a, b, f, h, s):
        low, high, far = zm * 2 + 1 - xh, zp * 2 + 1 - xh, z2 * 2 + 1 - xh
        mine = z2 * 2 + xh
        a.wait_recv()
        f2 = send(piece(low, 0), piece(low, 0), up)
        s.append(send(piece(low), piece(low), sibling))
        b.wait_recv()
        h2 = send(piece(high, 1), piece(high, 1), down)
        s.append(send(piece(high), piece(high), sibling))
        f.wait_recv()
        s.append(send(piece(mine, 0), piece(mine, 0), sibling))
        h.wait_recv()
        s.append(send(piece(mine, 1), piece(mine, 1), sibling))
        return f2, h2, far

    def fourth(piece, f2, h2, far, s):
        f2.wait_recv()
        s.append(send(piece(far, 0), piece(far, 0), sibling))
        h2.wait_recv()
        s.append(send(piece(far, 1), piece(far, 1), sibling))

    q_state = second(q_piece, q_x, q_u, q_d)
    o_state = second(o_piece, o_x, o_u, o_d)
    q_last = third(q_piece, *q_state)
    o_last = third(o_piece, *o_state)
    fourth(q_piece, *q_last, q_state[4])
    for copy in q_state[4]:
        copy.wait_recv()
    loads[3].wait()
    for copy in bias_copies:
        copy.wait_recv()
    bias_all[t] = bias_one[...]

    def project(i, carry):
        cols = pl.ds(pl.multiple_of(i * 256, 256), 256)
        q_f = jnp.dot(normed[...], q_all[:, cols], preferred_element_type=F32)
        for e in range(2):
            q_e = q_f[:, e * HEAD_DIM : (e + 1) * HEAD_DIM] + bias_all[2 * i + e][0:1]
            at = pl.ds(pl.multiple_of(i * 256 + e * HEAD_DIM, HEAD_DIM), HEAD_DIM)
            queries[:, at] = rotate(q_e, cos_rows, sin_rows).astype(BF16)
        return carry

    lax.fori_loop(0, HEADS // 2, project, 0)

    q_pos = lax.broadcasted_iota(jnp.int32, (SEQ, SEQ), 0)
    k_pos = lax.broadcasted_iota(jnp.int32, (SEQ, SEQ), 1)
    group = HEADS // KV_HEADS
    first_pair = ((y * 4 + xl * 2 + c) * 8 + t) * 2
    for p in range(2):
        rows = slice(p * SEQ, (p + 1) * SEQ)
        allowed = (k_pos <= q_pos) & (k_pos < lengths[first_pair + p])
        allowed = jnp.concatenate([allowed.astype(F32)] * group, axis=0) > 0.5
        for g in range(KV_HEADS):
            cols = slice(g * HEAD_DIM, (g + 1) * HEAD_DIM)
            q_g = jnp.concatenate(
                [
                    queries[rows, (g * group + h) * HEAD_DIM : (g * group + h + 1) * HEAD_DIM]
                    for h in range(group)
                ],
                axis=0,
            )
            logits = lax.dot_general(
                q_g, keys[rows, cols], (((1,), (1,)), ((), ())), preferred_element_type=F32
            ) / math.sqrt(HEAD_DIM)
            logits = jnp.where(allowed, logits, -1e30)
            shifted = jnp.exp(logits - jnp.max(logits, axis=-1, keepdims=True))
            probs = (shifted / jnp.sum(shifted, axis=-1, keepdims=True)).astype(BF16)
            ctx = jnp.dot(probs, values[rows, cols], preferred_element_type=F32).astype(BF16)
            for h in range(group):
                at = (g * group + h) * HEAD_DIM
                context[rows, at : at + HEAD_DIM] = ctx[h * SEQ : (h + 1) * SEQ]

    fourth(o_piece, *o_last, o_state[4])
    for copy in o_state[4]:
        copy.wait_recv()
    loads[4].wait()

    def project_out(i, carry):
        cols = pl.ds(pl.multiple_of(i * 256, 256), 256)
        attended = jnp.dot(context[...], o_all[:, cols], preferred_element_type=F32)
        base = x_v[:, :, cols].reshape(2 * SEQ, 256).astype(F32)
        after_out[:, cols] = (base + attended).astype(BF16)
        return carry

    lax.fori_loop(0, D // 256, project_out, 0)
    normed_out[...] = rms_rows(after_out[...].astype(F32), mlp_gain[...]).astype(BF16)
    send.drain()


def mlp_kernel(
    lengths, destination, final_gain, score_weight, normed, after, w_gate, w_up, w_down,
    relaid_out, scores_out,
    gathered, after_v, wg, wu, wd, w_tail, active, partial,
    r1_low, r1_high, r1_up, r1_down, r1_x, r2_x, r2_low, r2_high, r2_up, r2_down,
    staged, landed, last_rows, score_one, score_eight, score_sum, score_all,
    local_sem, send_sem, recv_sem,
):
    z, xh, c = lax.axis_index("z"), lax.axis_index("xh"), lax.axis_index("c")
    y, xl = lax.axis_index("y"), lax.axis_index("xl")
    t = z * 2 + xh
    b = y * 4 + xl * 2 + c
    partner = {"xh": 1 - xh}
    up, down = {"z": z_at(1)}, {"z": z_at(-1)}
    zp, zm, z2 = z_at(1), z_at(-1), z_at(2)

    loads = [
        pltpu.make_async_copy(normed, gathered.at[t], local_sem.at[0]),
        pltpu.make_async_copy(w_gate, wg, local_sem.at[1]),
        pltpu.make_async_copy(w_up, wu, local_sem.at[2]),
        pltpu.make_async_copy(w_down, wd.at[pl.ds(0, FFL)], local_sem.at[3]),
        pltpu.make_async_copy(after, after_v, local_sem.at[4]),
    ]
    for load in loads:
        load.start()
    greet([tensor_peer(k) for k in range(1, 8)] + [dp_peer(k)[1] for k in range(1, 16)])
    send = Sender(send_sem, recv_sem)

    def rows(g, span):
        return gathered.at[g, pl.ds(span[0], span[1] - span[0])]

    def pass_on(g, span, device):
        return send(rows(g, span), rows(g, span), device)

    here, there = t, z * 2 + 1 - xh
    low, high = zm * 2 + xh, zp * 2 + xh
    low_x, high_x = zm * 2 + 1 - xh, zp * 2 + 1 - xh
    far, far_x = z2 * 2 + xh, z2 * 2 + 1 - xh

    loads[0].wait()
    u2 = pass_on(here, C2, up)
    d2 = pass_on(here, C2, down)
    x1 = pass_on(here, C1, partner)
    u1 = pass_on(here, C1, up)
    d1 = pass_on(here, C1, down)
    x2 = pass_on(here, C2, partner)

    wd[FFL:FFP] = jnp.zeros((FFP - FFL, D), BF16)
    w_tail[...] = jnp.zeros_like(w_tail)
    loads[1].wait()
    w_tail[:, 0:TAIL] = wg[:, FULL:FFL]
    loads[2].wait()
    w_tail[:, 128 : 128 + TAIL] = wu[:, FULL:FFL]
    loads[3].wait()
    loads[4].wait()

    def gated(gate_values, up_values):
        return (gate_values / (1.0 + jnp.exp(-gate_values)) * up_values).astype(BF16)

    def block(g, own=False):
        def hidden(i, carry):
            cols = pl.ds(pl.multiple_of(i * 256, 256), 256)
            gate_values = jnp.dot(gathered[g], wg[:, cols], preferred_element_type=F32)
            up_values = jnp.dot(gathered[g], wu[:, cols], preferred_element_type=F32)
            active[:, cols] = gated(gate_values, up_values)
            return carry

        lax.fori_loop(0, FULL // 256, hidden, 0)
        both = jnp.dot(gathered[g], w_tail[...], preferred_element_type=F32)
        active[:, FULL:FFP] = gated(both[:, :128], both[:, 128:])

        def project(i, carry):
            cols = pl.ds(pl.multiple_of(i * 256, 256), 256)
            result = jnp.dot(active[...], wd[:, cols], preferred_element_type=F32)
            if own:
                result = result.astype(BF16).astype(F32) + after_v[:, cols].astype(F32)
            result = result.astype(BF16).reshape(2, 8, 16, 256)
            for owner in range(8):
                partial[owner, pl.ds(2 * g, 2), :, cols] = result[:, owner]
            return carry

        lax.fori_loop(0, D // 256, project, 0)

    block(here, own=True)
    u2.wait_recv()
    f2u = pass_on(low, C2A, up)
    x_low = pass_on(low, C2, partner)
    d2.wait_recv()
    f2d = pass_on(high, C2B, down)
    x_high = pass_on(high, C2, partner)
    x1.wait_recv()
    xu = pass_on(there, C1, up)
    xd = pass_on(there, C1, down)
    u1.wait_recv()
    f1u = pass_on(low, C1A, up)
    d1.wait_recv()
    f1d = pass_on(high, C1B, down)
    block(low)
    f2u.wait_recv()
    x_far_a = pass_on(far, C2A, partner)
    f2d.wait_recv()
    x_far_b = pass_on(far, C2B, partner)
    block(high)
    x2.wait_recv()
    block(there)
    xu.wait_recv()
    fxu = pass_on(low_x, C1A, up)
    xd.wait_recv()
    fxd = pass_on(high_x, C1B, down)
    x_low.wait_recv()
    block(low_x)
    x_high.wait_recv()
    block(high_x)
    f1u.wait_recv()
    f1d.wait_recv()
    block(far)
    fxu.wait_recv()
    fxd.wait_recv()
    x_far_a.wait_recv()
    x_far_b.wait_recv()
    block(far_x)

    def both_of(zz, lo, hi):
        return partial.at[pl.ds(2 * zz, 2), pl.ds(lo, hi - lo)]

    def one_of(index, lo, hi):
        return partial.at[index, pl.ds(lo, hi - lo)]

    a_up = send(both_of(z2, 0, N1A), r1_low, up)
    a_down = send(both_of(z2, N1A, N1), r1_high, down)
    sx = [
        send(one_of(zz * 2 + 1 - xh, N1, 16), r2_x.at[k], partner)
        for k, zz in enumerate((z2, zp, zm, z))
    ]

    def add_both(zz, lo, extra):
        def step(i, carry):
            for e in range(2):
                index = (2 * zz + e, lo + i)
                partial[index] = (partial[index].astype(F32) + extra[e, i].astype(F32)).astype(BF16)
            return carry

        lax.fori_loop(0, extra.shape[1], step, 0)

    def add_one(index, lo, extra, offset=0):
        def step(i, carry):
            at = (index, lo + i)
            partial[at] = (partial[at].astype(F32) + extra[i].astype(F32)).astype(BF16)
            return carry

        lax.fori_loop(0, extra.shape[0], step, 0)

    a_up.wait_recv()
    add_both(zp, 0, r1_low)
    b_up = send(both_of(zp, 0, N1), r1_up, up)
    a_down.wait_recv()
    add_both(zm, N1A, r1_high)
    b_down = send(both_of(zm, 0, N1), r1_down, down)

    sx[0].wait_recv()
    add_one(z2 * 2 + xh, N1, r2_x.at[0])
    c_up = send(one_of(z2 * 2 + xh, N1, N2A), r2_low, up)
    c_down = send(one_of(z2 * 2 + xh, N2A, 16), r2_high, down)
    sx[1].wait_recv()
    add_one(zp * 2 + xh, N1, r2_x.at[1])
    sx[2].wait_recv()
    add_one(zm * 2 + xh, N1, r2_x.at[2])

    b_up.wait_recv()
    b_down.wait_recv()

    def fold(i, carry):
        at = (z * 2 + 1 - xh, i)
        total = partial[at].astype(F32) + r1_up[1 - xh, i].astype(F32)
        partial[at] = (total + r1_down[1 - xh, i].astype(F32)).astype(BF16)
        return carry

    lax.fori_loop(0, N1, fold, 0)
    ex = send(one_of(z * 2 + 1 - xh, 0, N1), r1_x, partner)

    c_up.wait_recv()
    add_one(zp * 2 + xh, N1, r2_low)
    e_up = send(one_of(zp * 2 + xh, N1, 16), r2_up, up)
    c_down.wait_recv()
    add_one(zm * 2 + xh, N2A, r2_high)
    e_down = send(one_of(zm * 2 + xh, N1, 16), r2_down, down)
    sx[3].wait_recv()
    add_one(t, N1, r2_x.at[3])

    ex.wait_recv()

    def last_one(i, carry):
        total = partial[t, i].astype(F32) + r1_up[xh, i].astype(F32)
        total = total + r1_down[xh, i].astype(F32) + r1_x[i].astype(F32)
        partial[t, i] = total.astype(BF16)
        return carry

    lax.fori_loop(0, N1, last_one, 0)
    e_up.wait_recv()
    e_down.wait_recv()

    def last_two(i, carry):
        total = partial[t, N1 + i].astype(F32) + r2_up[i].astype(F32)
        partial[t, N1 + i] = (total + r2_down[i].astype(F32)).astype(BF16)
        return carry

    lax.fori_loop(0, 16 - N1, last_two, 0)

    pair_copies = []
    for k in range(16):
        index, device = dp_peer(k)
        pair = jnp.int32(0)
        for j in range(1, 16):
            pair = jnp.where(destination[b * 16 + j] == index, j, pair)
        if k == 0:
            landed[b] = partial[t, pair]
        else:
            staged[k] = partial[t, pair]
            pair_copies.append(send(staged.at[k], landed.at[b], device))

    position = lax.broadcasted_iota(jnp.int32, (16, D), 0)
    for p in range(16):
        wanted = lengths[b * 16 + p] - 1 - t * 16
        row = jnp.where(position == wanted, partial[t, p].astype(F32), 0.0)
        last_rows[p : p + 1] = jnp.sum(row, axis=0, keepdims=True)
    scored = rms_rows(last_rows[...], final_gain[...]) * score_weight[...]
    score_one[...] = jnp.broadcast_to(jnp.sum(scored, axis=-1, keepdims=True), score_one.shape)
    copies = [send(score_one, score_eight.at[t], tensor_peer(k)) for k in range(1, 8)]
    score_eight[t] = score_one[...]
    for copy in copies:
        copy.wait_recv()
    total = score_eight[0]
    for k in range(1, 8):
        total = total + score_eight[k]
    score_sum[...] = total
    score_all[b] = total
    copies = [send(score_sum, score_all.at[b], dp_peer(k)[1]) for k in range(1, 16)]
    for copy in copies:
        copy.wait_recv()
    scores_out[...] = score_all[...]
    for copy in pair_copies:
        copy.wait_recv()
    relaid_out[...] = landed[...]
    send.drain()


def any_spec():
    return pl.BlockSpec(memory_space=pl.ANY)


def vmem_spec():
    return pl.BlockSpec(memory_space=pltpu.VMEM)


def smem_spec():
    return pl.BlockSpec(memory_space=pltpu.SMEM)


def rotary_tables():
    index = np.arange(HEAD_DIM // 2, dtype=np.float32)
    frequency = np.power(np.float64(theta_base), -2.0 * index / HEAD_DIM).astype(np.float32)
    angles = np.arange(SEQ, dtype=np.float32)[:, None] * frequency[None, :]
    cosine, sine = np.cos(angles.astype(np.float64)), np.sin(angles.astype(np.float64))
    return (
        np.concatenate([cosine, cosine], axis=1).astype(np.float32),
        np.concatenate([-sine, sine], axis=1).astype(np.float32),
    )


def on_device(
    arrived, destination, query_of, lengths, attn_gain, q_weight, q_bias, k_weight, v_weight,
    v_bias, o_weight, mlp_gain, w_gate, w_up, w_down, final_gain, score_weight,
):
    cosine, sine = rotary_tables()
    row = lambda v: v.reshape(1, -1)
    after, normed = pl.pallas_call(
        attention_kernel,
        out_shape=[jax.ShapeDtypeStruct((2 * SEQ, D), BF16)] * 2,
        in_specs=[smem_spec()] + [vmem_spec()] * 6 + [any_spec()] * 5,
        out_specs=[vmem_spec()] * 2,
        scratch_shapes=[
            pltpu.VMEM((2, SEQ, D), BF16),
            pltpu.VMEM((D, KV_HEADS * HEAD_DIM), BF16),
            pltpu.VMEM((D, KV_HEADS * HEAD_DIM), BF16),
            pltpu.VMEM((D, HEADS * HEAD_DIM), BF16),
            pltpu.VMEM((HEADS * HEAD_DIM, D), BF16),
            pltpu.VMEM((8, HEAD_DIM), F32),
            pltpu.VMEM((8, 8, HEAD_DIM), F32),
            pltpu.VMEM((2 * SEQ, D), BF16),
            pltpu.VMEM((2 * SEQ, KV_HEADS * HEAD_DIM), BF16),
            pltpu.VMEM((2 * SEQ, KV_HEADS * HEAD_DIM), BF16),
            pltpu.VMEM((2 * SEQ, HEADS * HEAD_DIM), BF16),
            pltpu.VMEM((2 * SEQ, HEADS * HEAD_DIM), BF16),
            pltpu.SemaphoreType.DMA((5,)),
            pltpu.SemaphoreType.DMA((48,)),
            pltpu.SemaphoreType.DMA((48,)),
        ],
        compiler_params=pltpu.CompilerParams(
            collective_id=0, has_side_effects=True, vmem_limit_bytes=60 * 2**20
        ),
    )(
        lengths, row(attn_gain), row(mlp_gain), row(q_bias), row(v_bias), cosine, sine,
        arrived, q_weight, k_weight, v_weight, o_weight,
    )
    pairs = lambda *lead: pltpu.VMEM((*lead, 16, D), BF16)
    relaid, scores = pl.pallas_call(
        mlp_kernel,
        out_shape=[
            jax.ShapeDtypeStruct((16, 16, D), BF16),
            jax.ShapeDtypeStruct((16, 16, 128), F32),
        ],
        in_specs=[smem_spec()] * 2 + [vmem_spec()] * 2 + [any_spec()] * 5,
        out_specs=[vmem_spec()] * 2,
        scratch_shapes=[
            pltpu.VMEM((8, 2 * SEQ, D), BF16),
            pltpu.VMEM((2 * SEQ, D), BF16),
            pltpu.VMEM((D, FFL), BF16),
            pltpu.VMEM((D, FFL), BF16),
            pltpu.VMEM((FFP, D), BF16),
            pltpu.VMEM((D, 256), BF16),
            pltpu.VMEM((2 * SEQ, FFP), BF16),
            pairs(8, 16),
            pairs(2, N1A),
            pairs(2, N1 - N1A),
            pairs(2, N1),
            pairs(2, N1),
            pairs(N1),
            pairs(4, 16 - N1),
            pairs(N2A - N1),
            pairs(16 - N2A),
            pairs(16 - N1),
            pairs(16 - N1),
            pairs(16),
            pairs(16),
            pltpu.VMEM((16, D), F32),
            pltpu.VMEM((16, 128), F32),
            pltpu.VMEM((8, 16, 128), F32),
            pltpu.VMEM((16, 128), F32),
            pltpu.VMEM((16, 16, 128), F32),
            pltpu.SemaphoreType.DMA((5,)),
            pltpu.SemaphoreType.DMA((80,)),
            pltpu.SemaphoreType.DMA((80,)),
        ],
        compiler_params=pltpu.CompilerParams(
            collective_id=1, has_side_effects=True, vmem_limit_bytes=60 * 2**20
        ),
    )(
        lengths, destination, row(final_gain), row(score_weight), normed, after, w_gate, w_up,
        w_down,
    )
    hidden_out = jnp.transpose(relaid, (1, 0, 2))

    group_index = lax.axis_index(DP)
    pair_score = scores[:, :, 0].reshape(-1)
    query_total = lax.axis_size(DP) * QUERY_DP
    membership = query_of[:, None] == jnp.arange(query_total, dtype=jnp.int32)[None, :]
    means = jnp.sum(jnp.where(membership, pair_score[:, None], 0.0), axis=0) / (
        pair_score.shape[0] // query_total
    )
    own_mean = jnp.sum(jnp.where(membership, means[None, :], 0.0), axis=1)
    here = (destination == group_index).reshape(16, 16)
    centred = jnp.sum(jnp.where(here, (pair_score - own_mean).reshape(16, 16), 0.0), axis=1)
    query_mean = lax.dynamic_slice_in_dim(means, group_index * QUERY_DP, QUERY_DP)
    return (hidden_out, centred, query_mean)


def solution(mesh):
    split = Mesh(mesh.devices.reshape(4, 2, 2, 4, 2), AXES)
    placed = (
        P(DP + TENSOR, None, None),
        P(),
        P(),
        P(),
        P(),
        P(None, TENSOR),
        P(TENSOR),
        P(),
        P(),
        P(),
        P(TENSOR, None),
        P(),
        P(None, TENSOR),
        P(None, TENSOR),
        P(TENSOR, None),
        P(),
        P(),
    )
    return jax.shard_map(
        on_device,
        mesh=split,
        in_specs=placed,
        out_specs=(P(TENSOR, DP, None), P(DP), P(DP)),
        check_vma=False,
    )
```

```python
import functools
import math

import jax
import jax.numpy as jnp
import numpy as np
from jax import lax
from jax.experimental import pallas as pl
from jax.experimental.pallas import tpu as pltpu
from jax.sharding import Mesh
from jax.sharding import PartitionSpec as P

AXES = ("y", "xl", "c", "z", "xh")
DP = ("y", "xl", "c")
TENSOR = ("z", "xh")
MESH = pl.DeviceIdType.MESH
F32 = jnp.float32
BF16 = jnp.bfloat16

KV_HEADS = 2
HEAD_DIM = 128
HEADS = 8
QUERY_DP = 2
theta_base = 1000000.0
norm_eps = 1e-06

SEQ = 128
D = 1536
FFL = 1120
FULL = 1024
TAIL = FFL - FULL
FFP = 1152

C1 = (0, 144)
C1A, C1B = (0, 80), (80, 144)
C2 = (144, 256)
C2A, C2B = (144, 208), (208, 256)
N1, N1A = 9, 5
N2A = 13


def z_at(step):
    return lax.rem(lax.axis_index("z") + step + 4, 4)


class Sender:
    def __init__(self, send_sem, recv_sem):
        self.send_sem, self.recv_sem, self.count = send_sem, recv_sem, 0
        self.open = []

    def __call__(self, src, dst, device):
        i = self.count
        self.count += 1
        copy = pltpu.make_async_remote_copy(
            src_ref=src,
            dst_ref=dst,
            send_sem=self.send_sem.at[i],
            recv_sem=self.recv_sem.at[i],
            device_id=device,
            device_id_type=MESH,
        )
        copy.start()
        self.open.append(copy)
        return copy

    def drain(self):
        for copy in self.open:
            copy.wait_send()
        self.open = []


def tensor_peer(k):
    index = lax.rem(lax.axis_index("z") * 2 + lax.axis_index("xh") + k, 8)
    return {"z": index // 2, "xh": lax.rem(index, 2)}


def dp_peer(k):
    index = lax.axis_index("y") * 4 + lax.axis_index("xl") * 2 + lax.axis_index("c")
    index = lax.rem(index + k, 16)
    return index, {"y": index // 4, "xl": lax.rem(index // 2, 2), "c": lax.rem(index, 2)}


def greet(devices):
    barrier = pltpu.get_barrier_semaphore()
    for device in devices:
        pl.semaphore_signal(barrier, inc=1, device_id=device, device_id_type=MESH)
    pl.semaphore_wait(barrier, len(devices))


def rms_rows(values, gain):
    scale = lax.rsqrt(jnp.mean(values * values, axis=-1, keepdims=True) + norm_eps)
    return values * scale * gain


def rotate(values, cosine, sine):
    return values * cosine + pltpu.roll(values, HEAD_DIM // 2, 1) * sine


def layer_kernel(
    lengths, destination, gain, mlp_gain, final_gain, score_weight, q_bias, v_bias, cosine, sine,
    arrived, q_w, k_w, v_w, o_w, w_gate, w_up, w_down,
    relaid_out, scores_out,
    x_v, k_v, v_v, q_all, o_all, bias_one, bias_all, normed, keys, values, queries, context,
    after_v, gathered, wg, wu, wd, w_tail, active, partial,
    r1_low, r1_high, r1_up, r1_down, r1_x, r2_x, r2_low, r2_high, r2_up, r2_down,
    staged, landed, squares, dots, score_one, score_eight, score_sum, score_all,
    local_sem, send_sem, recv_sem,
):
    z, xh, c = lax.axis_index("z"), lax.axis_index("xh"), lax.axis_index("c")
    y, xl = lax.axis_index("y"), lax.axis_index("xl")
    t = z * 2 + xh
    b = y * 4 + xl * 2 + c
    partner, sibling = {"xh": 1 - xh}, {"c": 1 - c}
    up, down = {"z": z_at(1)}, {"z": z_at(-1)}
    zp, zm, z2 = z_at(1), z_at(-1), z_at(2)
    here, there = t, z * 2 + 1 - xh
    low, high = zm * 2 + xh, zp * 2 + xh
    low_x, high_x = zm * 2 + 1 - xh, zp * 2 + 1 - xh
    far, far_x = z2 * 2 + xh, z2 * 2 + 1 - xh

    def q_cols(index):
        return pl.ds(pl.multiple_of(index * HEAD_DIM, HEAD_DIM), HEAD_DIM)

    sources = [
        (arrived, x_v),
        (k_w, k_v),
        (v_w, v_v),
        (q_w, q_all.at[:, q_cols(t)]),
        (o_w, o_all.at[pl.ds(pl.multiple_of(t * HEAD_DIM, HEAD_DIM), HEAD_DIM)]),
        (w_gate, wg),
        (w_up, wu),
        (w_down, wd.at[pl.ds(0, FFL)]),
        (w_gate.at[pl.ds(FULL, TAIL)], w_tail.at[pl.ds(0, TAIL)]),
        (w_up.at[pl.ds(FULL, TAIL)], w_tail.at[pl.ds(128, TAIL)]),
    ]
    loads = [
        pltpu.make_async_copy(src, dst, local_sem.at[i]) for i, (src, dst) in enumerate(sources)
    ]
    for load in loads[:5]:
        load.start()
    bias_one[...] = jnp.broadcast_to(q_bias[...].reshape(1, HEAD_DIM).astype(F32), bias_one.shape)
    greet([tensor_peer(k) for k in range(1, 8)] + [dp_peer(k)[1] for k in range(1, 16)])
    send = Sender(send_sem, recv_sem)

    half_q, half_o = D // 2, HEAD_DIM // 2

    def q_piece(index, sub=None):
        size = half_q if sub is None else half_q // 2
        start = c * half_q + (0 if sub is None else sub * size)
        return q_all.at[pl.ds(pl.multiple_of(start, 128), size), q_cols(index)]

    def o_piece(index, sub=None):
        size = half_o if sub is None else half_o // 2
        start = index * HEAD_DIM + c * half_o + (0 if sub is None else sub * size)
        return o_all.at[pl.ds(pl.multiple_of(start, 32), size)]

    own_q = q_w.at[pl.ds(pl.multiple_of(c * half_q, 128), half_q)]
    own_o = o_w.at[pl.ds(pl.multiple_of(c * half_o, 64), half_o)]

    o_u, o_d = send(own_o, o_piece(t), up), send(own_o, o_piece(t), down)
    q_x = send(own_q, q_piece(t), partner)
    q_u, q_d = send(own_q, q_piece(t), up), send(own_q, q_piece(t), down)
    bias_copies = [send(bias_one, bias_all.at[t], tensor_peer(k)) for k in range(1, 8)]
    o_x = send(own_o, o_piece(t), partner)
    for load in loads[5:]:
        load.start()

    loads[0].wait()
    x = x_v[...].reshape(2 * SEQ, D)
    normed[...] = rms_rows(x.astype(F32), gain[...].reshape(1, D)).astype(BF16)
    loads[1].wait()
    loads[2].wait()
    cos_rows = jnp.concatenate([cosine[...]] * 2, axis=0)
    sin_rows = jnp.concatenate([sine[...]] * 2, axis=0)
    k_f = jnp.dot(normed[...], k_v[...], preferred_element_type=F32)
    for g in range(KV_HEADS):
        cols = slice(g * HEAD_DIM, (g + 1) * HEAD_DIM)
        keys[:, cols] = rotate(k_f[:, cols], cos_rows, sin_rows).astype(BF16)
    v_f = jnp.dot(normed[...], v_v[...], preferred_element_type=F32)
    values[...] = (v_f + v_bias[...].reshape(1, -1).astype(F32)).astype(BF16)

    q_sib, o_sib = [], []

    def share(piece, index, sub, copies):
        copies.append(send(piece(index, sub), piece(index, sub), sibling))

    def pass_piece(piece, index, sub, device):
        return send(piece(index, sub), piece(index, sub), device)

    o_u.wait_recv()
    o_fu = pass_piece(o_piece, low, 0, up)
    o_xl = pass_piece(o_piece, low, None, partner)
    share(o_piece, low, None, o_sib)
    o_d.wait_recv()
    o_fd = pass_piece(o_piece, high, 1, down)
    o_xh = pass_piece(o_piece, high, None, partner)
    share(o_piece, high, None, o_sib)
    q_x.wait_recv()
    q_xu = pass_piece(q_piece, there, None, up)
    q_xd = pass_piece(q_piece, there, None, down)
    share(q_piece, there, None, q_sib)
    q_u.wait_recv()
    q_fu = pass_piece(q_piece, low, 0, up)
    share(q_piece, low, None, q_sib)
    q_d.wait_recv()
    q_fd = pass_piece(q_piece, high, 1, down)
    share(q_piece, high, None, q_sib)
    o_fu.wait_recv()
    o_xfa = pass_piece(o_piece, far, 0, partner)
    share(o_piece, far, 0, o_sib)
    o_fd.wait_recv()
    o_xfb = pass_piece(o_piece, far, 1, partner)
    share(o_piece, far, 1, o_sib)
    o_x.wait_recv()
    share(o_piece, there, None, o_sib)
    q_xu.wait_recv()
    q_fxu = pass_piece(q_piece, low_x, 0, up)
    share(q_piece, low_x, None, q_sib)
    q_xd.wait_recv()
    q_fxd = pass_piece(q_piece, high_x, 1, down)
    share(q_piece, high_x, None, q_sib)
    o_xl.wait_recv()
    share(o_piece, low_x, None, o_sib)
    q_fu.wait_recv()
    share(q_piece, far, 0, q_sib)
    q_fd.wait_recv()
    share(q_piece, far, 1, q_sib)
    o_xh.wait_recv()
    share(o_piece, high_x, None, o_sib)
    q_fxu.wait_recv()
    share(q_piece, far_x, 0, q_sib)
    q_fxd.wait_recv()
    share(q_piece, far_x, 1, q_sib)
    for copy in q_sib:
        copy.wait_recv()
    loads[3].wait()
    for copy in bias_copies:
        copy.wait_recv()
    bias_all[t] = bias_one[...]

    def project_q(i, carry):
        cols = pl.ds(pl.multiple_of(i * 256, 256), 256)
        q_f = jnp.dot(normed[...], q_all[:, cols], preferred_element_type=F32)
        for e in range(2):
            q_e = q_f[:, e * HEAD_DIM : (e + 1) * HEAD_DIM] + bias_all[2 * i + e][0:1]
            at = pl.ds(pl.multiple_of(i * 256 + e * HEAD_DIM, HEAD_DIM), HEAD_DIM)
            queries[:, at] = rotate(q_e, cos_rows, sin_rows).astype(BF16)
        return carry

    lax.fori_loop(0, HEADS // 2, project_q, 0)

    o_xfa.wait_recv()
    share(o_piece, far_x, 0, o_sib)
    o_xfb.wait_recv()
    share(o_piece, far_x, 1, o_sib)

    q_pos = lax.broadcasted_iota(jnp.int32, (SEQ, SEQ), 0)
    k_pos = lax.broadcasted_iota(jnp.int32, (SEQ, SEQ), 1)
    group = HEADS // KV_HEADS
    first_pair = (b * 8 + t) * 2
    for p in range(2):
        rows = slice(p * SEQ, (p + 1) * SEQ)
        allowed = (k_pos <= q_pos) & (k_pos < lengths[first_pair + p])
        allowed = jnp.concatenate([allowed.astype(F32)] * group, axis=0) > 0.5
        for g in range(KV_HEADS):
            cols = slice(g * HEAD_DIM, (g + 1) * HEAD_DIM)
            q_g = jnp.concatenate(
                [
                    queries[rows, (g * group + h) * HEAD_DIM : (g * group + h + 1) * HEAD_DIM]
                    for h in range(group)
                ],
                axis=0,
            )
            logits = lax.dot_general(
                q_g, keys[rows, cols], (((1,), (1,)), ((), ())), preferred_element_type=F32
            ) / math.sqrt(HEAD_DIM)
            logits = jnp.where(allowed, logits, -1e30)
            shifted = jnp.exp(logits - jnp.max(logits, axis=-1, keepdims=True))
            probs = (shifted / jnp.sum(shifted, axis=-1, keepdims=True)).astype(BF16)
            ctx = jnp.dot(probs, values[rows, cols], preferred_element_type=F32).astype(BF16)
            for h in range(group):
                at = (g * group + h) * HEAD_DIM
                context[rows, at : at + HEAD_DIM] = ctx[h * SEQ : (h + 1) * SEQ]

    for copy in o_sib:
        copy.wait_recv()
    loads[4].wait()

    def project_out(i, carry):
        cols = pl.ds(pl.multiple_of(i * 256, 256), 256)
        attended = jnp.dot(context[...], o_all[:, cols], preferred_element_type=F32)
        base = x_v[:, :, cols].reshape(2 * SEQ, 256).astype(F32)
        after_v[:, cols] = (base + attended).astype(BF16)
        return carry

    lax.fori_loop(0, D // 256, project_out, 0)
    gathered[t] = rms_rows(after_v[...].astype(F32), mlp_gain[...].reshape(1, D)).astype(BF16)

    def block_rows(g, span):
        return gathered.at[g, pl.ds(span[0], span[1] - span[0])]

    def pass_on(g, span, device):
        return send(block_rows(g, span), block_rows(g, span), device)

    u2 = pass_on(here, C2, up)
    d2 = pass_on(here, C2, down)
    x1 = pass_on(here, C1, partner)
    u1 = pass_on(here, C1, up)
    d1 = pass_on(here, C1, down)
    x2 = pass_on(here, C2, partner)

    for load in loads[5:]:
        load.wait()
    wd[FFL:FFP] = jnp.zeros((FFP - FFL, D), BF16)
    w_tail[TAIL:128] = jnp.zeros((128 - TAIL, D), BF16)
    w_tail[128 + TAIL :] = jnp.zeros((128 - TAIL, D), BF16)

    def gated(gate_values, up_values):
        return (gate_values / (1.0 + jnp.exp(-gate_values)) * up_values).astype(BF16)

    def by_rows(g, weights):
        return lax.dot_general(
            gathered[g], weights, (((1,), (1,)), ((), ())), preferred_element_type=F32
        )

    def block(g, own=False):
        def hidden(i, carry):
            at = pl.ds(pl.multiple_of(i * 256, 256), 256)
            active[:, at] = gated(by_rows(g, wg[at]), by_rows(g, wu[at]))
            return carry

        lax.fori_loop(0, FULL // 256, hidden, 0)
        both = by_rows(g, w_tail[...])
        active[:, FULL:FFP] = gated(both[:, :128], both[:, 128:])

        def project(i, carry):
            cols = pl.ds(pl.multiple_of(i * 256, 256), 256)
            result = jnp.dot(active[...], wd[:, cols], preferred_element_type=F32)
            if own:
                result = result.astype(BF16).astype(F32) + after_v[:, cols].astype(F32)
            result = result.astype(BF16).reshape(2, 8, 16, 256)
            for owner in range(8):
                partial[owner, pl.ds(2 * g, 2), :, cols] = result[:, owner]
            return carry

        lax.fori_loop(0, D // 256, project, 0)

    block(here, own=True)
    u2.wait_recv()
    f2u = pass_on(low, C2A, up)
    x_low = pass_on(low, C2, partner)
    d2.wait_recv()
    f2d = pass_on(high, C2B, down)
    x_high = pass_on(high, C2, partner)
    x1.wait_recv()
    xu = pass_on(there, C1, up)
    xd = pass_on(there, C1, down)
    u1.wait_recv()
    f1u = pass_on(low, C1A, up)
    d1.wait_recv()
    f1d = pass_on(high, C1B, down)
    block(low)
    f2u.wait_recv()
    x_far_a = pass_on(far, C2A, partner)
    f2d.wait_recv()
    x_far_b = pass_on(far, C2B, partner)
    block(high)
    x2.wait_recv()
    block(there)
    xu.wait_recv()
    fxu = pass_on(low_x, C1A, up)
    xd.wait_recv()
    fxd = pass_on(high_x, C1B, down)
    x_low.wait_recv()
    block(low_x)
    x_high.wait_recv()
    block(high_x)
    f1u.wait_recv()
    f1d.wait_recv()
    block(far)
    fxu.wait_recv()
    fxd.wait_recv()
    x_far_a.wait_recv()
    x_far_b.wait_recv()
    block(far_x)

    def add_both(cols, zz, lo, extra):
        def step(i, carry):
            for e in range(2):
                at = (2 * zz + e, lo + i, slice(None), cols)
                partial[at] = (
                    partial[at].astype(F32) + extra[e, i, :, cols].astype(F32)
                ).astype(BF16)
            return carry

        lax.fori_loop(0, extra.shape[1], step, 0)

    def add_one(cols, index, lo, extra):
        def step(i, carry):
            at = (index, lo + i, slice(None), cols)
            partial[at] = (partial[at].astype(F32) + extra[i, :, cols].astype(F32)).astype(BF16)
            return carry

        lax.fori_loop(0, extra.shape[0], step, 0)

    class Half:
        def __init__(self, h):
            self.h = h
            self.cols = slice(h * (D // 2), (h + 1) * (D // 2))

        def both_of(self, zz, lo, hi):
            return partial.at[pl.ds(2 * zz, 2), pl.ds(lo, hi - lo), :, self.cols]

        def one_of(self, index, lo, hi):
            return partial.at[index, pl.ds(lo, hi - lo), :, self.cols]

        def begin(self):
            cols = self.cols
            self.a_up = send(self.both_of(z2, 0, N1A), r1_low.at[:, :, :, cols], up)
            self.a_down = send(self.both_of(z2, N1A, N1), r1_high.at[:, :, :, cols], down)

        def cross(self, k):
            zz = (z2, zp, zm, z)[k]
            return send(
                self.one_of(zz * 2 + 1 - xh, N1, 16), r2_x.at[k, :, :, self.cols], partner
            )

        def middle(self):
            cols = self.cols
            self.a_up.wait_recv()
            add_both(cols, zp, 0, r1_low)
            self.b_up = send(self.both_of(zp, 0, N1), r1_up.at[:, :, :, cols], up)
            self.a_down.wait_recv()
            add_both(cols, zm, N1A, r1_high)
            self.b_down = send(self.both_of(zm, 0, N1), r1_down.at[:, :, :, cols], down)

        def second(self, sx):
            cols = self.cols
            sx[0].wait_recv()
            add_one(cols, far, N1, r2_x.at[0])
            self.c_up = send(self.one_of(far, N1, N2A), r2_low.at[:, :, cols], up)
            self.c_down = send(self.one_of(far, N2A, 16), r2_high.at[:, :, cols], down)
            sx[1].wait_recv()
            add_one(cols, high, N1, r2_x.at[1])
            sx[2].wait_recv()
            add_one(cols, low, N1, r2_x.at[2])

        def third(self):
            cols = self.cols
            self.c_up.wait_recv()
            add_one(cols, high, N1, r2_low)
            self.e_up = send(self.one_of(high, N1, 16), r2_up.at[:, :, cols], up)
            self.c_down.wait_recv()
            add_one(cols, low, N2A, r2_high)
            self.e_down = send(self.one_of(low, N1, 16), r2_down.at[:, :, cols], down)

        def fold(self):
            cols = self.cols
            self.b_up.wait_recv()
            self.b_down.wait_recv()

            def step(i, carry):
                at = (there, i, slice(None), cols)
                total = partial[at].astype(F32) + r1_up[1 - xh, i, :, cols].astype(F32)
                partial[at] = (total + r1_down[1 - xh, i, :, cols].astype(F32)).astype(BF16)
                return carry

            lax.fori_loop(0, N1, step, 0)
            self.ex = send(self.one_of(there, 0, N1), r1_x.at[:, :, cols], partner)

        def finish(self, sx):
            cols = self.cols
            sx[3].wait_recv()
            add_one(cols, t, N1, r2_x.at[3])
            self.e_up.wait_recv()
            self.e_down.wait_recv()

            def two(i, carry):
                at = (t, N1 + i, slice(None), cols)
                total = partial[at].astype(F32) + r2_up[i, :, cols].astype(F32)
                partial[at] = (total + r2_down[i, :, cols].astype(F32)).astype(BF16)
                return carry

            lax.fori_loop(0, 16 - N1, two, 0)
            self.ex.wait_recv()

            def one(i, carry):
                at = (t, i, slice(None), cols)
                total = partial[at].astype(F32) + r1_up[xh, i, :, cols].astype(F32)
                total = total + r1_down[xh, i, :, cols].astype(F32)
                partial[at] = (total + r1_x[i, :, cols].astype(F32)).astype(BF16)
                return carry

            lax.fori_loop(0, N1, one, 0)

        def relay(self):
            cols = self.cols
            copies = []
            for k in range(16):
                device = dp_peer(k)[1]
                if k == 0:
                    landed[b, :, cols] = partial[t, chosen[k], :, cols]
                else:
                    staged[k, :, cols] = partial[t, chosen[k], :, cols]
                    copies.append(
                        send(staged.at[k, :, cols], landed.at[b, :, cols], device)
                    )
            return copies

        def score(self):
            cols = self.cols
            weight = (final_gain[...] * score_weight[...]).reshape(1, D)[:, cols]
            position = lax.broadcasted_iota(jnp.int32, (16, D // 2), 0)
            for p in range(16):
                wanted = lengths[b * 16 + p] - 1 - t * 16
                row = jnp.where(position == wanted, partial[t, p, :, cols].astype(F32), 0.0)
                row = jnp.sum(row, axis=0, keepdims=True)
                sums = jnp.sum(row * row, axis=-1, keepdims=True)
                squares[self.h, p : p + 1] = jnp.broadcast_to(sums, (1, 128))
                sums = jnp.sum(row * weight, axis=-1, keepdims=True)
                dots[self.h, p : p + 1] = jnp.broadcast_to(sums, (1, 128))

    chosen = []
    for k in range(16):
        index = dp_peer(k)[0]
        pair = jnp.int32(0)
        for j in range(1, 16):
            pair = jnp.where(destination[b * 16 + j] == index, j, pair)
        chosen.append(pair)

    h0, h1 = Half(0), Half(1)
    h0.begin()
    sx0 = [h0.cross(k) for k in range(4)]
    h1.begin()
    sx1 = [h1.cross(0)]
    h0.middle()
    h0.second(sx0)
    h0.third()
    h0.fold()
    sx1 += [h1.cross(k) for k in range(1, 4)]
    h1.middle()
    h0.finish(sx0)
    pair_copies = h0.relay()
    h0.score()
    h1.second(sx1)
    h1.third()
    h1.fold()
    h1.finish(sx1)
    pair_copies += h1.relay()
    h1.score()

    mean = (squares[0] + squares[1]) / D
    score_one[...] = (dots[0] + dots[1]) * lax.rsqrt(mean + norm_eps)
    copies = [send(score_one, score_eight.at[t], tensor_peer(k)) for k in range(1, 8)]
    score_eight[t] = score_one[...]
    for copy in copies:
        copy.wait_recv()
    total = score_eight[0]
    for k in range(1, 8):
        total = total + score_eight[k]
    score_sum[...] = total
    score_all[b] = total
    copies = [send(score_sum, score_all.at[b], dp_peer(k)[1]) for k in range(1, 16)]
    for copy in copies:
        copy.wait_recv()
    scores_out[...] = score_all[...]
    for copy in pair_copies:
        copy.wait_recv()
    relaid_out[...] = landed[...]
    send.drain()


def any_spec():
    return pl.BlockSpec(memory_space=pl.ANY)


def vmem_spec():
    return pl.BlockSpec(memory_space=pltpu.VMEM)


def smem_spec():
    return pl.BlockSpec(memory_space=pltpu.SMEM)


def rotary_tables():
    index = np.arange(HEAD_DIM // 2, dtype=np.float32)
    frequency = np.power(np.float64(theta_base), -2.0 * index / HEAD_DIM).astype(np.float32)
    angles = np.arange(SEQ, dtype=np.float32)[:, None] * frequency[None, :]
    cosine, sine = np.cos(angles.astype(np.float64)), np.sin(angles.astype(np.float64))
    return (
        np.concatenate([cosine, cosine], axis=1).astype(np.float32),
        np.concatenate([-sine, sine], axis=1).astype(np.float32),
    )


def on_device(
    arrived, destination, query_of, lengths, attn_gain, q_weight, q_bias, k_weight, v_weight,
    v_bias, o_weight, mlp_gain, w_gate, w_up, w_down, final_gain, score_weight,
):
    cosine, sine = rotary_tables()
    pairs = lambda *lead: pltpu.VMEM((*lead, 16, D), BF16)
    relaid, scores = pl.pallas_call(
        layer_kernel,
        out_shape=[
            jax.ShapeDtypeStruct((16, 16, D), BF16),
            jax.ShapeDtypeStruct((16, 16, 128), F32),
        ],
        in_specs=[smem_spec()] * 2 + [vmem_spec()] * 8 + [any_spec()] * 8,
        out_specs=[vmem_spec()] * 2,
        scratch_shapes=[
            pltpu.VMEM((2, SEQ, D), BF16),
            pltpu.VMEM((D, KV_HEADS * HEAD_DIM), BF16),
            pltpu.VMEM((D, KV_HEADS * HEAD_DIM), BF16),
            pltpu.VMEM((D, HEADS * HEAD_DIM), BF16),
            pltpu.VMEM((HEADS * HEAD_DIM, D), BF16),
            pltpu.VMEM((8, HEAD_DIM), F32),
            pltpu.VMEM((8, 8, HEAD_DIM), F32),
            pltpu.VMEM((2 * SEQ, D), BF16),
            pltpu.VMEM((2 * SEQ, KV_HEADS * HEAD_DIM), BF16),
            pltpu.VMEM((2 * SEQ, KV_HEADS * HEAD_DIM), BF16),
            pltpu.VMEM((2 * SEQ, HEADS * HEAD_DIM), BF16),
            pltpu.VMEM((2 * SEQ, HEADS * HEAD_DIM), BF16),
            pltpu.VMEM((2 * SEQ, D), BF16),
            pltpu.VMEM((8, 2 * SEQ, D), BF16),
            pltpu.VMEM((FFL, D), BF16),
            pltpu.VMEM((FFL, D), BF16),
            pltpu.VMEM((FFP, D), BF16),
            pltpu.VMEM((256, D), BF16),
            pltpu.VMEM((2 * SEQ, FFP), BF16),
            pairs(8, 16),
            pairs(2, N1A),
            pairs(2, N1 - N1A),
            pairs(2, N1),
            pairs(2, N1),
            pairs(N1),
            pairs(4, 16 - N1),
            pairs(N2A - N1),
            pairs(16 - N2A),
            pairs(16 - N1),
            pairs(16 - N1),
            pairs(16),
            pairs(16),
            pltpu.VMEM((2, 16, 128), F32),
            pltpu.VMEM((2, 16, 128), F32),
            pltpu.VMEM((16, 128), F32),
            pltpu.VMEM((8, 16, 128), F32),
            pltpu.VMEM((16, 128), F32),
            pltpu.VMEM((16, 16, 128), F32),
            pltpu.SemaphoreType.DMA((10,)),
            pltpu.SemaphoreType.DMA((144,)),
            pltpu.SemaphoreType.DMA((144,)),
        ],
        compiler_params=pltpu.CompilerParams(
            collective_id=0, has_side_effects=True, vmem_limit_bytes=60 * 2**20
        ),
    )(
        lengths, destination, attn_gain, mlp_gain, final_gain, score_weight, q_bias, v_bias,
        cosine, sine, arrived, q_weight, k_weight, v_weight, o_weight, w_gate.T, w_up.T, w_down,
    )
    hidden_out = jnp.transpose(relaid, (1, 0, 2))

    group_index = lax.axis_index(DP)
    pair_score = scores[:, :, 0].reshape(-1)
    query_total = lax.axis_size(DP) * QUERY_DP
    membership = query_of[:, None] == jnp.arange(query_total, dtype=jnp.int32)[None, :]
    means = jnp.sum(jnp.where(membership, pair_score[:, None], 0.0), axis=0) / (
        pair_score.shape[0] // query_total
    )
    own_mean = jnp.sum(jnp.where(membership, means[None, :], 0.0), axis=1)
    here = (destination == group_index).reshape(16, 16)
    centred = jnp.sum(jnp.where(here, (pair_score - own_mean).reshape(16, 16), 0.0), axis=1)
    query_mean = lax.dynamic_slice_in_dim(means, group_index * QUERY_DP, QUERY_DP)
    return (hidden_out, centred, query_mean)


def solution(mesh):
    split = Mesh(mesh.devices.reshape(4, 2, 2, 4, 2), AXES)
    placed = (
        P(DP + TENSOR, None, None),
        P(),
        P(),
        P(),
        P(),
        P(None, TENSOR),
        P(TENSOR),
        P(),
        P(),
        P(),
        P(TENSOR, None),
        P(),
        P(None, TENSOR),
        P(None, TENSOR),
        P(TENSOR, None),
        P(),
        P(),
    )
    return jax.shard_map(
        on_device,
        mesh=split,
        in_specs=placed,
        out_specs=(P(TENSOR, DP, None), P(DP), P(DP)),
        check_vma=False,
    )
```

```python
import functools
import math

import jax
import jax.numpy as jnp
import numpy as np
from jax import lax
from jax.experimental import pallas as pl
from jax.experimental.pallas import tpu as pltpu
from jax.sharding import Mesh
from jax.sharding import PartitionSpec as P

AXES = ("y", "xl", "c", "z", "xh")
DP = ("y", "xl", "c")
TENSOR = ("z", "xh")
MESH = pl.DeviceIdType.MESH
F32 = jnp.float32
BF16 = jnp.bfloat16

KV_HEADS = 2
HEAD_DIM = 128
HEADS = 8
QUERY_DP = 2
theta_base = 1000000.0
norm_eps = 1e-06

SEQ = 128
D = 1536
FFL = 1120
FULL = 1024
TAIL = FFL - FULL
FFP = 1152

C1 = (0, 144)
C1A, C1B = (0, 80), (80, 144)
C2 = (144, 256)
C2A, C2B = (144, 208), (208, 256)
N1, N1A = 9, 5
N2A = 13


ORDER = (
    ("x2", 0), ("x3", 0), ("b", 0), ("x0", 0), ("x1", 0), ("x2", 1), ("b", 1), ("md", 0),
    ("mu", 0), ("s0", 0), ("x1", 1), ("md", 1), ("x0", 1), ("mu", 1), ("fo", 0), ("s0", 1),
    ("s2", 1), ("s1", 0), ("s3", 0), ("tu", 0), ("s2", 0), ("td", 0), ("x3", 1), ("s1", 1),
    ("td", 1), ("fo", 1), ("tu", 1), ("s3", 1), ("f1", 0), ("f2", 0), ("re", 0), ("sc", 0),
    ("f1", 1), ("f2", 1), ("re", 1), ("sc", 1),
)


def z_at(step):
    return lax.rem(lax.axis_index("z") + step + 4, 4)


class Sender:
    def __init__(self, send_sem, recv_sem):
        self.send_sem, self.recv_sem, self.count = send_sem, recv_sem, 0
        self.open = []

    def __call__(self, src, dst, device):
        i = self.count
        self.count += 1
        copy = pltpu.make_async_remote_copy(
            src_ref=src,
            dst_ref=dst,
            send_sem=self.send_sem.at[i],
            recv_sem=self.recv_sem.at[i],
            device_id=device,
            device_id_type=MESH,
        )
        copy.start()
        self.open.append(copy)
        return copy

    def drain(self):
        for copy in self.open:
            copy.wait_send()
        self.open = []


def tensor_peer(k):
    index = lax.rem(lax.axis_index("z") * 2 + lax.axis_index("xh") + k, 8)
    return {"z": index // 2, "xh": lax.rem(index, 2)}


def dp_peer(k):
    index = lax.axis_index("y") * 4 + lax.axis_index("xl") * 2 + lax.axis_index("c")
    index = lax.rem(index + k, 16)
    return index, {"y": index // 4, "xl": lax.rem(index // 2, 2), "c": lax.rem(index, 2)}


def greet(devices):
    barrier = pltpu.get_barrier_semaphore()
    for device in devices:
        pl.semaphore_signal(barrier, inc=1, device_id=device, device_id_type=MESH)
    pl.semaphore_wait(barrier, len(devices))


def rms_rows(values, gain):
    scale = lax.rsqrt(jnp.mean(values * values, axis=-1, keepdims=True) + norm_eps)
    return values * scale * gain


def rotate(values, cosine, sine):
    return values * cosine + pltpu.roll(values, HEAD_DIM // 2, 1) * sine


def layer_kernel(
    lengths, destination, gain, mlp_gain, final_gain, score_weight, q_bias, v_bias, cosine, sine,
    arrived, q_w, k_w, v_w, o_w, w_gate, w_up, w_down,
    relaid_out, scores_out,
    x_v, k_v, v_v, q_all, o_all, bias_one, bias_all, normed, keys, values, queries, context,
    after_v, gathered, wg, wu, wd, w_tail, active, partial,
    r1_low, r1_high, r1_up, r1_down, r1_x, r2_x, r2_low, r2_high, r2_up, r2_down,
    staged, landed, squares, dots, score_one, score_eight, score_sum, score_all,
    local_sem, send_sem, recv_sem,
):
    z, xh, c = lax.axis_index("z"), lax.axis_index("xh"), lax.axis_index("c")
    y, xl = lax.axis_index("y"), lax.axis_index("xl")
    t = z * 2 + xh
    b = y * 4 + xl * 2 + c
    partner, sibling = {"xh": 1 - xh}, {"c": 1 - c}
    up, down = {"z": z_at(1)}, {"z": z_at(-1)}
    zp, zm, z2 = z_at(1), z_at(-1), z_at(2)
    here, there = t, z * 2 + 1 - xh
    low, high = zm * 2 + xh, zp * 2 + xh
    low_x, high_x = zm * 2 + 1 - xh, zp * 2 + 1 - xh
    far, far_x = z2 * 2 + xh, z2 * 2 + 1 - xh

    def q_cols(index):
        return pl.ds(pl.multiple_of(index * HEAD_DIM, HEAD_DIM), HEAD_DIM)

    sources = [
        (arrived, x_v),
        (k_w, k_v),
        (v_w, v_v),
        (q_w, q_all.at[:, q_cols(t)]),
        (o_w, o_all.at[pl.ds(pl.multiple_of(t * HEAD_DIM, HEAD_DIM), HEAD_DIM)]),
        (w_gate, wg),
        (w_up, wu),
        (w_down, wd.at[pl.ds(0, FFL)]),
        (w_gate.at[pl.ds(FULL, TAIL)], w_tail.at[pl.ds(0, TAIL)]),
        (w_up.at[pl.ds(FULL, TAIL)], w_tail.at[pl.ds(128, TAIL)]),
    ]
    loads = [
        pltpu.make_async_copy(src, dst, local_sem.at[i]) for i, (src, dst) in enumerate(sources)
    ]
    for load in loads[:5]:
        load.start()
    bias_one[...] = jnp.broadcast_to(q_bias[...].reshape(1, HEAD_DIM).astype(F32), bias_one.shape)
    greet([tensor_peer(k) for k in range(1, 8)] + [dp_peer(k)[1] for k in range(1, 16)])
    send = Sender(send_sem, recv_sem)

    half_q, half_o = D // 2, HEAD_DIM // 2

    def q_piece(index, sub=None):
        size = half_q if sub is None else half_q // 2
        start = c * half_q + (0 if sub is None else sub * size)
        return q_all.at[pl.ds(pl.multiple_of(start, 128), size), q_cols(index)]

    def o_piece(index, sub=None):
        size = half_o if sub is None else half_o // 2
        start = index * HEAD_DIM + c * half_o + (0 if sub is None else sub * size)
        return o_all.at[pl.ds(pl.multiple_of(start, 32), size)]

    own_q = q_w.at[pl.ds(pl.multiple_of(c * half_q, 128), half_q)]
    own_o = o_w.at[pl.ds(pl.multiple_of(c * half_o, 64), half_o)]

    o_u, o_d = send(own_o, o_piece(t), up), send(own_o, o_piece(t), down)
    q_x = send(own_q, q_piece(t), partner)
    q_u, q_d = send(own_q, q_piece(t), up), send(own_q, q_piece(t), down)
    bias_copies = [send(bias_one, bias_all.at[t], tensor_peer(k)) for k in range(1, 8)]
    o_x = send(own_o, o_piece(t), partner)
    for load in loads[5:]:
        load.start()

    loads[0].wait()
    x = x_v[...].reshape(2 * SEQ, D)
    normed[...] = rms_rows(x.astype(F32), gain[...].reshape(1, D)).astype(BF16)
    loads[1].wait()
    loads[2].wait()
    cos_rows = jnp.concatenate([cosine[...]] * 2, axis=0)
    sin_rows = jnp.concatenate([sine[...]] * 2, axis=0)
    k_f = jnp.dot(normed[...], k_v[...], preferred_element_type=F32)
    for g in range(KV_HEADS):
        cols = slice(g * HEAD_DIM, (g + 1) * HEAD_DIM)
        keys[:, cols] = rotate(k_f[:, cols], cos_rows, sin_rows).astype(BF16)
    v_f = jnp.dot(normed[...], v_v[...], preferred_element_type=F32)
    values[...] = (v_f + v_bias[...].reshape(1, -1).astype(F32)).astype(BF16)

    q_sib, o_sib = [], []

    def share(piece, index, sub, copies):
        copies.append(send(piece(index, sub), piece(index, sub), sibling))

    def pass_piece(piece, index, sub, device):
        return send(piece(index, sub), piece(index, sub), device)

    o_u.wait_recv()
    o_fu = pass_piece(o_piece, low, 0, up)
    o_xl = pass_piece(o_piece, low, None, partner)
    share(o_piece, low, None, o_sib)
    o_d.wait_recv()
    o_fd = pass_piece(o_piece, high, 1, down)
    o_xh = pass_piece(o_piece, high, None, partner)
    share(o_piece, high, None, o_sib)
    q_x.wait_recv()
    q_xu = pass_piece(q_piece, there, None, up)
    q_xd = pass_piece(q_piece, there, None, down)
    share(q_piece, there, None, q_sib)
    q_u.wait_recv()
    q_fu = pass_piece(q_piece, low, 0, up)
    share(q_piece, low, None, q_sib)
    q_d.wait_recv()
    q_fd = pass_piece(q_piece, high, 1, down)
    share(q_piece, high, None, q_sib)
    o_fu.wait_recv()
    o_xfa = pass_piece(o_piece, far, 0, partner)
    share(o_piece, far, 0, o_sib)
    o_fd.wait_recv()
    o_xfb = pass_piece(o_piece, far, 1, partner)
    share(o_piece, far, 1, o_sib)
    o_x.wait_recv()
    share(o_piece, there, None, o_sib)
    q_xu.wait_recv()
    q_fxu = pass_piece(q_piece, low_x, 0, up)
    share(q_piece, low_x, None, q_sib)
    q_xd.wait_recv()
    q_fxd = pass_piece(q_piece, high_x, 1, down)
    share(q_piece, high_x, None, q_sib)
    o_xl.wait_recv()
    share(o_piece, low_x, None, o_sib)
    q_fu.wait_recv()
    share(q_piece, far, 0, q_sib)
    q_fd.wait_recv()
    share(q_piece, far, 1, q_sib)
    o_xh.wait_recv()
    share(o_piece, high_x, None, o_sib)
    q_fxu.wait_recv()
    share(q_piece, far_x, 0, q_sib)
    q_fxd.wait_recv()
    share(q_piece, far_x, 1, q_sib)
    for copy in q_sib:
        copy.wait_recv()
    loads[3].wait()
    for copy in bias_copies:
        copy.wait_recv()
    bias_all[t] = bias_one[...]

    def project_q(i, carry):
        cols = pl.ds(pl.multiple_of(i * 256, 256), 256)
        q_f = jnp.dot(normed[...], q_all[:, cols], preferred_element_type=F32)
        for e in range(2):
            q_e = q_f[:, e * HEAD_DIM : (e + 1) * HEAD_DIM] + bias_all[2 * i + e][0:1]
            at = pl.ds(pl.multiple_of(i * 256 + e * HEAD_DIM, HEAD_DIM), HEAD_DIM)
            queries[:, at] = rotate(q_e, cos_rows, sin_rows).astype(BF16)
        return carry

    lax.fori_loop(0, HEADS // 2, project_q, 0, unroll=True)

    o_xfa.wait_recv()
    share(o_piece, far_x, 0, o_sib)
    o_xfb.wait_recv()
    share(o_piece, far_x, 1, o_sib)

    q_pos = lax.broadcasted_iota(jnp.int32, (SEQ, SEQ), 0)
    k_pos = lax.broadcasted_iota(jnp.int32, (SEQ, SEQ), 1)
    group = HEADS // KV_HEADS
    first_pair = (b * 8 + t) * 2
    for p in range(2):
        rows = slice(p * SEQ, (p + 1) * SEQ)
        allowed = (k_pos <= q_pos) & (k_pos < lengths[first_pair + p])
        allowed = jnp.concatenate([allowed.astype(F32)] * group, axis=0) > 0.5
        for g in range(KV_HEADS):
            cols = slice(g * HEAD_DIM, (g + 1) * HEAD_DIM)
            q_g = jnp.concatenate(
                [
                    queries[rows, (g * group + h) * HEAD_DIM : (g * group + h + 1) * HEAD_DIM]
                    for h in range(group)
                ],
                axis=0,
            )
            logits = lax.dot_general(
                q_g, keys[rows, cols], (((1,), (1,)), ((), ())), preferred_element_type=F32
            ) / math.sqrt(HEAD_DIM)
            logits = jnp.where(allowed, logits, -1e30)
            shifted = jnp.exp(logits - jnp.max(logits, axis=-1, keepdims=True))
            probs = (shifted / jnp.sum(shifted, axis=-1, keepdims=True)).astype(BF16)
            ctx = jnp.dot(probs, values[rows, cols], preferred_element_type=F32).astype(BF16)
            for h in range(group):
                at = (g * group + h) * HEAD_DIM
                context[rows, at : at + HEAD_DIM] = ctx[h * SEQ : (h + 1) * SEQ]

    for copy in o_sib:
        copy.wait_recv()
    loads[4].wait()

    def project_out(i, carry):
        cols = pl.ds(pl.multiple_of(i * 256, 256), 256)
        attended = jnp.dot(context[...], o_all[:, cols], preferred_element_type=F32)
        base = x_v[:, :, cols].reshape(2 * SEQ, 256).astype(F32)
        after_v[:, cols] = (base + attended).astype(BF16)
        return carry

    lax.fori_loop(0, D // 256, project_out, 0, unroll=True)
    gathered[t] = rms_rows(after_v[...].astype(F32), mlp_gain[...].reshape(1, D)).astype(BF16)

    def block_rows(g, span):
        return gathered.at[g, pl.ds(span[0], span[1] - span[0])]

    def pass_on(g, span, device):
        return send(block_rows(g, span), block_rows(g, span), device)

    u2 = pass_on(here, C2, up)
    d2 = pass_on(here, C2, down)
    x1 = pass_on(here, C1, partner)
    u1 = pass_on(here, C1, up)
    d1 = pass_on(here, C1, down)
    x2 = pass_on(here, C2, partner)

    for load in loads[5:]:
        load.wait()
    wd[FFL:FFP] = jnp.zeros((FFP - FFL, D), BF16)
    w_tail[TAIL:128] = jnp.zeros((128 - TAIL, D), BF16)
    w_tail[128 + TAIL :] = jnp.zeros((128 - TAIL, D), BF16)

    def gated(gate_values, up_values):
        return (gate_values / (1.0 + jnp.exp(-gate_values)) * up_values).astype(BF16)

    def by_rows(g, weights):
        return lax.dot_general(
            gathered[g], weights, (((1,), (1,)), ((), ())), preferred_element_type=F32
        )

    def block(g, own=False):
        def hidden(i, carry):
            at = pl.ds(pl.multiple_of(i * 256, 256), 256)
            active[:, at] = gated(by_rows(g, wg[at]), by_rows(g, wu[at]))
            return carry

        lax.fori_loop(0, FULL // 256, hidden, 0, unroll=True)
        both = by_rows(g, w_tail[...])
        active[:, FULL:FFP] = gated(both[:, :128], both[:, 128:])

        def project(i, carry):
            cols = pl.ds(pl.multiple_of(i * 256, 256), 256)
            result = jnp.dot(active[...], wd[:, cols], preferred_element_type=F32)
            if own:
                result = result.astype(BF16).astype(F32) + after_v[:, cols].astype(F32)
            result = result.astype(BF16).reshape(2, 8, 16, 256)
            for owner in range(8):
                partial[owner, pl.ds(2 * g, 2), :, cols] = result[:, owner]
            return carry

        lax.fori_loop(0, D // 256, project, 0, unroll=True)

    block(here, own=True)
    u2.wait_recv()
    f2u = pass_on(low, C2A, up)
    x_low = pass_on(low, C2, partner)
    d2.wait_recv()
    f2d = pass_on(high, C2B, down)
    x_high = pass_on(high, C2, partner)
    x1.wait_recv()
    xu = pass_on(there, C1, up)
    xd = pass_on(there, C1, down)
    u1.wait_recv()
    f1u = pass_on(low, C1A, up)
    d1.wait_recv()
    f1d = pass_on(high, C1B, down)
    block(low)
    f2u.wait_recv()
    x_far_a = pass_on(far, C2A, partner)
    f2d.wait_recv()
    x_far_b = pass_on(far, C2B, partner)
    block(high)
    x2.wait_recv()
    block(there)
    xu.wait_recv()
    fxu = pass_on(low_x, C1A, up)
    xd.wait_recv()
    fxd = pass_on(high_x, C1B, down)
    x_low.wait_recv()
    block(low_x)
    x_high.wait_recv()
    block(high_x)
    f1u.wait_recv()
    f1d.wait_recv()
    block(far)
    fxu.wait_recv()
    fxd.wait_recv()
    x_far_a.wait_recv()
    x_far_b.wait_recv()
    block(far_x)

    def add_both(cols, zz, lo, extra):
        def step(i, carry):
            for e in range(2):
                at = (2 * zz + e, lo + i, slice(None), cols)
                partial[at] = (
                    partial[at].astype(F32) + extra[e, i, :, cols].astype(F32)
                ).astype(BF16)
            return carry

        lax.fori_loop(0, extra.shape[1], step, 0, unroll=True)

    def add_one(cols, index, lo, extra):
        def step(i, carry):
            at = (index, lo + i, slice(None), cols)
            partial[at] = (partial[at].astype(F32) + extra[i, :, cols].astype(F32)).astype(BF16)
            return carry

        lax.fori_loop(0, extra.shape[0], step, 0, unroll=True)

    class Half:
        def __init__(self, h):
            self.h, self.sx, self.copies = h, [None] * 4, []
            self.cols = slice(h * (D // 2), (h + 1) * (D // 2))

        def both_of(self, zz, lo, hi):
            return partial.at[pl.ds(2 * zz, 2), pl.ds(lo, hi - lo), :, self.cols]

        def one_of(self, index, lo, hi):
            return partial.at[index, pl.ds(lo, hi - lo), :, self.cols]

        def begin(self):
            cols = self.cols
            self.a_up = send(self.both_of(z2, 0, N1A), r1_low.at[:, :, :, cols], up)
            self.a_down = send(self.both_of(z2, N1A, N1), r1_high.at[:, :, :, cols], down)

        def cross(self, k):
            zz = (z2, zp, zm, z)[k]
            self.sx[k] = send(
                self.one_of(zz * 2 + 1 - xh, N1, 16), r2_x.at[k, :, :, self.cols], partner
            )

        def mid_up(self):
            self.a_up.wait_recv()
            add_both(self.cols, zp, 0, r1_low)
            self.b_up = send(self.both_of(zp, 0, N1), r1_up.at[:, :, :, self.cols], up)

        def mid_down(self):
            self.a_down.wait_recv()
            add_both(self.cols, zm, N1A, r1_high)
            self.b_down = send(self.both_of(zm, 0, N1), r1_down.at[:, :, :, self.cols], down)

        def crossed(self, k):
            self.sx[k].wait_recv()
            add_one(self.cols, (far, high, low, t)[k], N1, r2_x.at[k])
            if k == 0:
                cols = self.cols
                self.c_up = send(self.one_of(far, N1, N2A), r2_low.at[:, :, cols], up)
                self.c_down = send(self.one_of(far, N2A, 16), r2_high.at[:, :, cols], down)

        def third_up(self):
            self.c_up.wait_recv()
            add_one(self.cols, high, N1, r2_low)
            self.e_up = send(self.one_of(high, N1, 16), r2_up.at[:, :, self.cols], up)

        def third_down(self):
            self.c_down.wait_recv()
            add_one(self.cols, low, N2A, r2_high)
            self.e_down = send(self.one_of(low, N1, 16), r2_down.at[:, :, self.cols], down)

        def fold(self):
            cols = self.cols
            self.b_up.wait_recv()
            self.b_down.wait_recv()

            def step(i, carry):
                at = (there, i, slice(None), cols)
                total = partial[at].astype(F32) + r1_up[1 - xh, i, :, cols].astype(F32)
                partial[at] = (total + r1_down[1 - xh, i, :, cols].astype(F32)).astype(BF16)
                return carry

            lax.fori_loop(0, N1, step, 0, unroll=3)
            self.ex = send(self.one_of(there, 0, N1), r1_x.at[:, :, cols], partner)

        def finish_two(self):
            cols = self.cols
            self.e_up.wait_recv()
            self.e_down.wait_recv()

            def step(i, carry):
                at = (t, N1 + i, slice(None), cols)
                total = partial[at].astype(F32) + r2_up[i, :, cols].astype(F32)
                partial[at] = (total + r2_down[i, :, cols].astype(F32)).astype(BF16)
                return carry

            lax.fori_loop(0, 16 - N1, step, 0, unroll=True)

        def finish_one(self):
            cols = self.cols
            self.ex.wait_recv()

            def step(i, carry):
                at = (t, i, slice(None), cols)
                total = partial[at].astype(F32) + r1_up[xh, i, :, cols].astype(F32)
                total = total + r1_down[xh, i, :, cols].astype(F32)
                partial[at] = (total + r1_x[i, :, cols].astype(F32)).astype(BF16)
                return carry

            lax.fori_loop(0, N1, step, 0, unroll=3)

        def relay(self):
            cols = self.cols
            for k in range(16):
                device = dp_peer(k)[1]
                if k == 0:
                    landed[b, :, cols] = partial[t, chosen[k], :, cols]
                else:
                    staged[k, :, cols] = partial[t, chosen[k], :, cols]
                    self.copies.append(
                        send(staged.at[k, :, cols], landed.at[b, :, cols], device)
                    )

        def score(self):
            cols = self.cols
            weight = (final_gain[...] * score_weight[...]).reshape(1, D)[:, cols]
            position = lax.broadcasted_iota(jnp.int32, (16, D // 2), 0)
            for p in range(16):
                wanted = lengths[b * 16 + p] - 1 - t * 16
                row = jnp.where(position == wanted, partial[t, p, :, cols].astype(F32), 0.0)
                row = jnp.sum(row, axis=0, keepdims=True)
                sums = jnp.sum(row * row, axis=-1, keepdims=True)
                squares[self.h, p : p + 1] = jnp.broadcast_to(sums, (1, 128))
                sums = jnp.sum(row * weight, axis=-1, keepdims=True)
                dots[self.h, p : p + 1] = jnp.broadcast_to(sums, (1, 128))

    chosen = []
    for k in range(16):
        index = dp_peer(k)[0]
        pair = jnp.int32(0)
        for j in range(1, 16):
            pair = jnp.where(destination[b * 16 + j] == index, j, pair)
        chosen.append(pair)

    halves = (Half(0), Half(1))
    steps = {
        "b": Half.begin,
        "mu": Half.mid_up,
        "md": Half.mid_down,
        "tu": Half.third_up,
        "td": Half.third_down,
        "fo": Half.fold,
        "f2": Half.finish_two,
        "f1": Half.finish_one,
        "re": Half.relay,
        "sc": Half.score,
    }
    for k in range(4):
        steps[f"x{k}"] = functools.partial(Half.cross, k=k)
        steps[f"s{k}"] = functools.partial(Half.crossed, k=k)
    for name, h in ORDER:
        steps[name](halves[h])
    pair_copies = halves[0].copies + halves[1].copies

    mean = (squares[0] + squares[1]) / D
    score_one[...] = (dots[0] + dots[1]) * lax.rsqrt(mean + norm_eps)
    copies = [send(score_one, score_eight.at[t], tensor_peer(k)) for k in range(1, 8)]
    score_eight[t] = score_one[...]
    for copy in copies:
        copy.wait_recv()
    total = score_eight[0]
    for k in range(1, 8):
        total = total + score_eight[k]
    score_sum[...] = total
    score_all[b] = total
    copies = [send(score_sum, score_all.at[b], dp_peer(k)[1]) for k in range(1, 16)]
    for copy in copies:
        copy.wait_recv()
    scores_out[...] = score_all[...]
    for copy in pair_copies:
        copy.wait_recv()
    relaid_out[...] = landed[...]
    send.drain()


def any_spec():
    return pl.BlockSpec(memory_space=pl.ANY)


def vmem_spec():
    return pl.BlockSpec(memory_space=pltpu.VMEM)


def smem_spec():
    return pl.BlockSpec(memory_space=pltpu.SMEM)


def rotary_tables():
    index = np.arange(HEAD_DIM // 2, dtype=np.float32)
    frequency = np.power(np.float64(theta_base), -2.0 * index / HEAD_DIM).astype(np.float32)
    angles = np.arange(SEQ, dtype=np.float32)[:, None] * frequency[None, :]
    cosine, sine = np.cos(angles.astype(np.float64)), np.sin(angles.astype(np.float64))
    return (
        np.concatenate([cosine, cosine], axis=1).astype(np.float32),
        np.concatenate([-sine, sine], axis=1).astype(np.float32),
    )


def on_device(
    arrived, destination, query_of, lengths, attn_gain, q_weight, q_bias, k_weight, v_weight,
    v_bias, o_weight, mlp_gain, w_gate, w_up, w_down, final_gain, score_weight,
):
    cosine, sine = rotary_tables()
    pairs = lambda *lead: pltpu.VMEM((*lead, 16, D), BF16)
    relaid, scores = pl.pallas_call(
        layer_kernel,
        out_shape=[
            jax.ShapeDtypeStruct((16, 16, D), BF16),
            jax.ShapeDtypeStruct((16, 16, 128), F32),
        ],
        in_specs=[smem_spec()] * 2 + [vmem_spec()] * 8 + [any_spec()] * 8,
        out_specs=[vmem_spec()] * 2,
        scratch_shapes=[
            pltpu.VMEM((2, SEQ, D), BF16),
            pltpu.VMEM((D, KV_HEADS * HEAD_DIM), BF16),
            pltpu.VMEM((D, KV_HEADS * HEAD_DIM), BF16),
            pltpu.VMEM((D, HEADS * HEAD_DIM), BF16),
            pltpu.VMEM((HEADS * HEAD_DIM, D), BF16),
            pltpu.VMEM((8, HEAD_DIM), F32),
            pltpu.VMEM((8, 8, HEAD_DIM), F32),
            pltpu.VMEM((2 * SEQ, D), BF16),
            pltpu.VMEM((2 * SEQ, KV_HEADS * HEAD_DIM), BF16),
            pltpu.VMEM((2 * SEQ, KV_HEADS * HEAD_DIM), BF16),
            pltpu.VMEM((2 * SEQ, HEADS * HEAD_DIM), BF16),
            pltpu.VMEM((2 * SEQ, HEADS * HEAD_DIM), BF16),
            pltpu.VMEM((2 * SEQ, D), BF16),
            pltpu.VMEM((8, 2 * SEQ, D), BF16),
            pltpu.VMEM((FFL, D), BF16),
            pltpu.VMEM((FFL, D), BF16),
            pltpu.VMEM((FFP, D), BF16),
            pltpu.VMEM((256, D), BF16),
            pltpu.VMEM((2 * SEQ, FFP), BF16),
            pairs(8, 16),
            pairs(2, N1A),
            pairs(2, N1 - N1A),
            pairs(2, N1),
            pairs(2, N1),
            pairs(N1),
            pairs(4, 16 - N1),
            pairs(N2A - N1),
            pairs(16 - N2A),
            pairs(16 - N1),
            pairs(16 - N1),
            pairs(16),
            pairs(16),
            pltpu.VMEM((2, 16, 128), F32),
            pltpu.VMEM((2, 16, 128), F32),
            pltpu.VMEM((16, 128), F32),
            pltpu.VMEM((8, 16, 128), F32),
            pltpu.VMEM((16, 128), F32),
            pltpu.VMEM((16, 16, 128), F32),
            pltpu.SemaphoreType.DMA((10,)),
            pltpu.SemaphoreType.DMA((144,)),
            pltpu.SemaphoreType.DMA((144,)),
        ],
        compiler_params=pltpu.CompilerParams(
            collective_id=0, has_side_effects=True, vmem_limit_bytes=60 * 2**20
        ),
    )(
        lengths, destination, attn_gain, mlp_gain, final_gain, score_weight, q_bias, v_bias,
        cosine, sine, arrived, q_weight, k_weight, v_weight, o_weight, w_gate.T, w_up.T, w_down,
    )
    hidden_out = jnp.transpose(relaid, (1, 0, 2))

    group_index = lax.axis_index(DP)
    pair_score = scores[:, :, 0].reshape(-1)
    query_total = lax.axis_size(DP) * QUERY_DP
    membership = query_of[:, None] == jnp.arange(query_total, dtype=jnp.int32)[None, :]
    means = jnp.sum(jnp.where(membership, pair_score[:, None], 0.0), axis=0) / (
        pair_score.shape[0] // query_total
    )
    own_mean = jnp.sum(jnp.where(membership, means[None, :], 0.0), axis=1)
    here = (destination == group_index).reshape(16, 16)
    centred = jnp.sum(jnp.where(here, (pair_score - own_mean).reshape(16, 16), 0.0), axis=1)
    query_mean = lax.dynamic_slice_in_dim(means, group_index * QUERY_DP, QUERY_DP)
    return (hidden_out, centred, query_mean)


def solution(mesh):
    split = Mesh(mesh.devices.reshape(4, 2, 2, 4, 2), AXES)
    placed = (
        P(DP + TENSOR, None, None),
        P(),
        P(),
        P(),
        P(),
        P(None, TENSOR),
        P(TENSOR),
        P(),
        P(),
        P(),
        P(TENSOR, None),
        P(),
        P(None, TENSOR),
        P(None, TENSOR),
        P(TENSOR, None),
        P(),
        P(),
    )
    return jax.shard_map(
        on_device,
        mesh=split,
        in_specs=placed,
        out_specs=(P(TENSOR, DP, None), P(DP), P(DP)),
        check_vma=False,
    )
```

```python
import functools
import math

import jax
import jax.numpy as jnp
import numpy as np
from jax import lax
from jax.experimental import pallas as pl
from jax.experimental.pallas import tpu as pltpu
from jax.sharding import Mesh
from jax.sharding import PartitionSpec as P

AXES = ("y", "xl", "c", "z", "xh")
DP = ("y", "xl", "c")
TENSOR = ("z", "xh")
MESH = pl.DeviceIdType.MESH
F32 = jnp.float32
BF16 = jnp.bfloat16

KV_HEADS = 2
HEAD_DIM = 128
HEADS = 8
QUERY_DP = 2
theta_base = 1000000.0
norm_eps = 1e-06

SEQ = 128
D = 1536
FFL = 1120
FULL = 1024
TAIL = FFL - FULL
FFP = 1152

C1 = (0, 144)
C1A, C1B = (0, 80), (80, 144)
C2 = (144, 256)
C2A, C2B = (144, 208), (208, 256)
N1, N1A = 9, 5
N2A = 13


ORDER = (
    ("x2", 0), ("x3", 0), ("b", 0), ("x0", 0), ("x1", 0), ("x2", 1), ("b", 1), ("md", 0),
    ("mu", 0), ("s0", 0), ("x1", 1), ("md", 1), ("x0", 1), ("mu", 1), ("fo", 0), ("s0", 1),
    ("s2", 1), ("s1", 0), ("s3", 0), ("tu", 0), ("s2", 0), ("td", 0), ("x3", 1), ("s1", 1),
    ("td", 1), ("fo", 1), ("tu", 1), ("s3", 1), ("f1", 0), ("f2", 0), ("re", 0), ("sc", 0),
    ("f1", 1), ("f2", 1), ("sc", 1),
)


EARLY = 5


def z_at(step):
    return lax.rem(lax.axis_index("z") + step + 4, 4)


class Sender:
    def __init__(self, send_sem, recv_sem):
        self.send_sem, self.recv_sem, self.count = send_sem, recv_sem, 0
        self.open = []

    def __call__(self, src, dst, device):
        i = self.count
        self.count += 1
        copy = pltpu.make_async_remote_copy(
            src_ref=src,
            dst_ref=dst,
            send_sem=self.send_sem.at[i],
            recv_sem=self.recv_sem.at[i],
            device_id=device,
            device_id_type=MESH,
        )
        copy.start()
        self.open.append(copy)
        return copy

    def drain(self):
        for copy in self.open:
            copy.wait_send()
        self.open = []


def tensor_peer(k):
    index = lax.rem(lax.axis_index("z") * 2 + lax.axis_index("xh") + k, 8)
    return {"z": index // 2, "xh": lax.rem(index, 2)}


def dp_peer(k):
    index = lax.axis_index("y") * 4 + lax.axis_index("xl") * 2 + lax.axis_index("c")
    index = lax.rem(index + k, 16)
    return index, {"y": index // 4, "xl": lax.rem(index // 2, 2), "c": lax.rem(index, 2)}


def rms_rows(values, gain):
    scale = lax.rsqrt(jnp.mean(values * values, axis=-1, keepdims=True) + norm_eps)
    return values * scale * gain


def rotate(values, cosine, sine):
    return values * cosine + pltpu.roll(values, HEAD_DIM // 2, 1) * sine


def layer_kernel(
    lengths, destination, q_bias, v_bias,
    gain_in, mlp_gain_in, final_gain_in, score_weight_in, cosine_in, sine_in,
    arrived, q_w, k_w, v_w, o_w, w_gate, w_up, w_down,
    relaid_out, scores_out,
    gain, mlp_gain, final_gain, score_weight, cosine, sine,
    x_v, k_v, v_v, q_all, o_all, bias_one, bias_all, normed, keys, values, queries, context,
    after_v, gathered, wg, wu, wd, w_tail, active, partial,
    r1_low, r1_high, r1_up, r1_down, r1_x, r2_x, r2_low, r2_high, r2_up, r2_down,
    staged, landed, last_rows, squares, dots, score_one, score_eight, score_sum, score_all,
    local_sem, send_sem, recv_sem,
):
    z, xh, c = lax.axis_index("z"), lax.axis_index("xh"), lax.axis_index("c")
    y, xl = lax.axis_index("y"), lax.axis_index("xl")
    t = z * 2 + xh
    b = y * 4 + xl * 2 + c
    partner, sibling = {"xh": 1 - xh}, {"c": 1 - c}
    up, down = {"z": z_at(1)}, {"z": z_at(-1)}
    zp, zm, z2 = z_at(1), z_at(-1), z_at(2)
    here, there = t, z * 2 + 1 - xh
    low, high = zm * 2 + xh, zp * 2 + xh
    low_x, high_x = zm * 2 + 1 - xh, zp * 2 + 1 - xh
    far, far_x = z2 * 2 + xh, z2 * 2 + 1 - xh

    def q_cols(index):
        return pl.ds(pl.multiple_of(index * HEAD_DIM, HEAD_DIM), HEAD_DIM)

    sources = [
        (arrived, x_v),
        (k_w, k_v),
        (v_w, v_v),
        (q_w, q_all.at[:, q_cols(t)]),
        (o_w, o_all.at[pl.ds(pl.multiple_of(t * HEAD_DIM, HEAD_DIM), HEAD_DIM)]),
        (w_gate, wg),
        (w_up, wu),
        (w_down, wd.at[pl.ds(0, FFL)]),
        (w_gate.at[pl.ds(FULL, TAIL)], w_tail.at[pl.ds(0, TAIL)]),
        (w_up.at[pl.ds(FULL, TAIL)], w_tail.at[pl.ds(128, TAIL)]),
        (gain_in, gain),
        (cosine_in, cosine),
        (sine_in, sine),
        (mlp_gain_in, mlp_gain),
        (final_gain_in, final_gain),
        (score_weight_in, score_weight),
    ]
    loads = [
        pltpu.make_async_copy(src, dst, local_sem.at[i]) for i, (src, dst) in enumerate(sources)
    ]
    peers = [tensor_peer(k) for k in range(1, 8)] + [dp_peer(k)[1] for k in range(1, 16)]
    barrier = pltpu.get_barrier_semaphore()
    for device in peers:
        pl.semaphore_signal(barrier, inc=1, device_id=device, device_id_type=MESH)
    for i in (3, 4, 0, 1, 2, *range(10, 16)):
        loads[i].start()
    bias_one[...] = jnp.broadcast_to(q_bias[...].reshape(1, HEAD_DIM).astype(F32), bias_one.shape)
    pl.semaphore_wait(barrier, len(peers))
    send = Sender(send_sem, recv_sem)

    half_q, half_o = D // 2, HEAD_DIM // 2

    def q_piece(index, sub=None):
        size = half_q if sub is None else half_q // 2
        start = c * half_q + (0 if sub is None else sub * size)
        return q_all.at[pl.ds(pl.multiple_of(start, 128), size), q_cols(index)]

    def o_piece(index, sub=None):
        size = half_o if sub is None else half_o // 2
        start = index * HEAD_DIM + c * half_o + (0 if sub is None else sub * size)
        return o_all.at[pl.ds(pl.multiple_of(start, 32), size)]

    own_q, own_o = q_piece(t), o_piece(t)
    loads[3].wait()
    loads[4].wait()

    o_u, o_d = send(own_o, o_piece(t), up), send(own_o, o_piece(t), down)
    q_x = send(own_q, q_piece(t), partner)
    q_u, q_d = send(own_q, q_piece(t), up), send(own_q, q_piece(t), down)
    bias_copies = [send(bias_one, bias_all.at[t], tensor_peer(k)) for k in range(1, 8)]
    o_x = send(own_o, o_piece(t), partner)
    for load in loads[5:10]:
        load.start()

    loads[0].wait()
    for load in loads[10:]:
        load.wait()
    x = x_v[...].reshape(2 * SEQ, D)
    normed[...] = rms_rows(x.astype(F32), gain[...].reshape(1, D)).astype(BF16)
    loads[1].wait()
    loads[2].wait()
    cos_rows = jnp.concatenate([cosine[...]] * 2, axis=0)
    sin_rows = jnp.concatenate([sine[...]] * 2, axis=0)
    k_f = jnp.dot(normed[...], k_v[...], preferred_element_type=F32)
    for g in range(KV_HEADS):
        cols = slice(g * HEAD_DIM, (g + 1) * HEAD_DIM)
        keys[:, cols] = rotate(k_f[:, cols], cos_rows, sin_rows).astype(BF16)
    v_f = jnp.dot(normed[...], v_v[...], preferred_element_type=F32)
    values[...] = (v_f + v_bias[...].reshape(1, -1).astype(F32)).astype(BF16)

    q_sib, o_sib = [], []

    def project_q(i):
        cols = pl.ds(pl.multiple_of(i * 256, 256), 256)
        q_f = jnp.dot(normed[...], q_all[:, cols], preferred_element_type=F32)
        for e in range(2):
            q_e = q_f[:, e * HEAD_DIM : (e + 1) * HEAD_DIM] + bias_all[2 * i + e][0:1]
            at = pl.ds(pl.multiple_of(i * 256 + e * HEAD_DIM, HEAD_DIM), HEAD_DIM)
            queries[:, at] = rotate(q_e, cos_rows, sin_rows).astype(BF16)

    def share(piece, index, sub, copies):
        copies.append(send(piece(index, sub), piece(index, sub), sibling))

    def pass_piece(piece, index, sub, device):
        return send(piece(index, sub), piece(index, sub), device)

    o_u.wait_recv()
    o_fu = pass_piece(o_piece, low, 0, up)
    o_xl = pass_piece(o_piece, low, None, partner)
    share(o_piece, low, None, o_sib)
    o_d.wait_recv()
    o_fd = pass_piece(o_piece, high, 1, down)
    o_xh = pass_piece(o_piece, high, None, partner)
    share(o_piece, high, None, o_sib)
    q_x.wait_recv()
    q_xu = pass_piece(q_piece, there, None, up)
    q_xd = pass_piece(q_piece, there, None, down)
    share(q_piece, there, None, q_sib)
    q_u.wait_recv()
    q_fu = pass_piece(q_piece, low, 0, up)
    share(q_piece, low, None, q_sib)
    q_d.wait_recv()
    q_fd = pass_piece(q_piece, high, 1, down)
    share(q_piece, high, None, q_sib)
    o_fu.wait_recv()
    o_xfa = pass_piece(o_piece, far, 0, partner)
    share(o_piece, far, 0, o_sib)
    o_fd.wait_recv()
    o_xfb = pass_piece(o_piece, far, 1, partner)
    share(o_piece, far, 1, o_sib)
    o_x.wait_recv()
    share(o_piece, there, None, o_sib)
    for copy in bias_copies:
        copy.wait_recv()
    bias_all[t] = bias_one[...]
    q_sib[0].wait_recv()
    project_q(z)
    q_xu.wait_recv()
    q_fxu = pass_piece(q_piece, low_x, 0, up)
    share(q_piece, low_x, None, q_sib)
    q_xd.wait_recv()
    q_fxd = pass_piece(q_piece, high_x, 1, down)
    share(q_piece, high_x, None, q_sib)
    o_xl.wait_recv()
    share(o_piece, low_x, None, o_sib)
    q_fu.wait_recv()
    share(q_piece, far, 0, q_sib)
    q_fd.wait_recv()
    share(q_piece, far, 1, q_sib)
    o_xh.wait_recv()
    share(o_piece, high_x, None, o_sib)
    for copy in q_sib[1:5]:
        copy.wait_recv()
    project_q(zm)
    project_q(zp)
    q_fxu.wait_recv()
    share(q_piece, far_x, 0, q_sib)
    q_fxd.wait_recv()
    share(q_piece, far_x, 1, q_sib)
    for copy in q_sib[5:]:
        copy.wait_recv()
    project_q(z2)

    o_xfa.wait_recv()
    share(o_piece, far_x, 0, o_sib)
    o_xfb.wait_recv()
    share(o_piece, far_x, 1, o_sib)

    q_pos = lax.broadcasted_iota(jnp.int32, (SEQ, SEQ), 0)
    k_pos = lax.broadcasted_iota(jnp.int32, (SEQ, SEQ), 1)
    group = HEADS // KV_HEADS
    first_pair = (b * 8 + t) * 2
    for copy in o_sib:
        copy.wait_recv()

    def attend(p):
        rows = slice(p * SEQ, (p + 1) * SEQ)
        allowed = (k_pos <= q_pos) & (k_pos < lengths[first_pair + p])
        allowed = jnp.concatenate([allowed.astype(F32)] * group, axis=0) > 0.5
        for g in range(KV_HEADS):
            cols = slice(g * HEAD_DIM, (g + 1) * HEAD_DIM)
            q_g = jnp.concatenate(
                [
                    queries[rows, (g * group + h) * HEAD_DIM : (g * group + h + 1) * HEAD_DIM]
                    for h in range(group)
                ],
                axis=0,
            )
            logits = lax.dot_general(
                q_g, keys[rows, cols], (((1,), (1,)), ((), ())), preferred_element_type=F32
            ) / math.sqrt(HEAD_DIM)
            logits = jnp.where(allowed, logits, -1e30)
            shifted = jnp.exp(logits - jnp.max(logits, axis=-1, keepdims=True))
            probs = (shifted / jnp.sum(shifted, axis=-1, keepdims=True)).astype(BF16)
            ctx = jnp.dot(probs, values[rows, cols], preferred_element_type=F32).astype(BF16)
            for h in range(group):
                at = (g * group + h) * HEAD_DIM
                context[rows, at : at + HEAD_DIM] = ctx[h * SEQ : (h + 1) * SEQ]
        for i in range(D // 256):
            cols = slice(i * 256, (i + 1) * 256)
            attended = jnp.dot(context[rows], o_all[:, cols], preferred_element_type=F32)
            after_v[rows, cols] = (x_v[p, :, cols].astype(F32) + attended).astype(BF16)
        after_rows = after_v[rows].astype(F32)
        gathered[t, rows] = rms_rows(after_rows, mlp_gain[...].reshape(1, D)).astype(BF16)

    def block_rows(g, span):
        return gathered.at[g, pl.ds(span[0], span[1] - span[0])]

    def pass_on(g, span, device):
        return send(block_rows(g, span), block_rows(g, span), device)

    attend(1)
    u2 = pass_on(here, C2, up)
    d2 = pass_on(here, C2, down)
    x2 = pass_on(here, C2, partner)
    attend(0)
    u1 = pass_on(here, C1, up)
    d1 = pass_on(here, C1, down)
    x1 = pass_on(here, C1, partner)

    for load in loads[5:10]:
        load.wait()
    wd[FFL:FFP] = jnp.zeros((FFP - FFL, D), BF16)
    w_tail[TAIL:128] = jnp.zeros((128 - TAIL, D), BF16)
    w_tail[128 + TAIL :] = jnp.zeros((128 - TAIL, D), BF16)

    def gated(gate_values, up_values):
        return (gate_values / (1.0 + jnp.exp(-gate_values)) * up_values).astype(BF16)

    def by_rows(g, weights):
        return lax.dot_general(
            gathered[g], weights, (((1,), (1,)), ((), ())), preferred_element_type=F32
        )

    def block(g, own=False, between=None):
        def hidden(i, carry):
            at = pl.ds(pl.multiple_of(i * 256, 256), 256)
            active[:, at] = gated(by_rows(g, wg[at]), by_rows(g, wu[at]))
            return carry

        lax.fori_loop(0, FULL // 256, hidden, 0, unroll=True)
        both = by_rows(g, w_tail[...])
        active[:, FULL:FFP] = gated(both[:, :128], both[:, 128:])

        for i in range(D // 256):
            if i == D // 512 and between is not None:
                between()
            cols = slice(i * 256, (i + 1) * 256)
            result = jnp.dot(active[...], wd[:, cols], preferred_element_type=F32)
            if own:
                result = result.astype(BF16).astype(F32) + after_v[:, cols].astype(F32)
            result = result.astype(BF16).reshape(2, 8, 16, 256)
            for owner in range(8):
                partial[owner, pl.ds(2 * g, 2), :, cols] = result[:, owner]

    block(here, own=True)
    u2.wait_recv()
    f2u = pass_on(low, C2A, up)
    x_low = pass_on(low, C2, partner)
    d2.wait_recv()
    f2d = pass_on(high, C2B, down)
    x_high = pass_on(high, C2, partner)
    x1.wait_recv()
    xu = pass_on(there, C1, up)
    xd = pass_on(there, C1, down)
    u1.wait_recv()
    f1u = pass_on(low, C1A, up)
    d1.wait_recv()
    f1d = pass_on(high, C1B, down)
    block(low)
    f2u.wait_recv()
    x_far_a = pass_on(far, C2A, partner)
    f2d.wait_recv()
    x_far_b = pass_on(far, C2B, partner)
    block(high)
    x2.wait_recv()
    block(there)
    xu.wait_recv()
    fxu = pass_on(low_x, C1A, up)
    xd.wait_recv()
    fxd = pass_on(high_x, C1B, down)
    x_low.wait_recv()
    block(low_x)
    x_high.wait_recv()
    block(high_x)
    f1u.wait_recv()
    f1d.wait_recv()
    block(far)
    fxu.wait_recv()
    fxd.wait_recv()
    x_far_a.wait_recv()
    x_far_b.wait_recv()

    def add_both(cols, zz, lo, extra):
        def step(i, carry):
            for e in range(2):
                at = (2 * zz + e, lo + i, slice(None), cols)
                partial[at] = (
                    partial[at].astype(F32) + extra[e, i, :, cols].astype(F32)
                ).astype(BF16)
            return carry

        lax.fori_loop(0, extra.shape[1], step, 0, unroll=True)

    def add_one(cols, index, lo, extra):
        def step(i, carry):
            at = (index, lo + i, slice(None), cols)
            partial[at] = (partial[at].astype(F32) + extra[i, :, cols].astype(F32)).astype(BF16)
            return carry

        lax.fori_loop(0, extra.shape[0], step, 0, unroll=True)

    class Half:
        def __init__(self, h):
            self.h, self.sx, self.copies = h, [None] * 4, []
            self.cols = slice(h * (D // 2), (h + 1) * (D // 2))

        def both_of(self, zz, lo, hi):
            return partial.at[pl.ds(2 * zz, 2), pl.ds(lo, hi - lo), :, self.cols]

        def one_of(self, index, lo, hi):
            return partial.at[index, pl.ds(lo, hi - lo), :, self.cols]

        def begin(self):
            cols = self.cols
            self.a_up = send(self.both_of(z2, 0, N1A), r1_low.at[:, :, :, cols], up)
            self.a_down = send(self.both_of(z2, N1A, N1), r1_high.at[:, :, :, cols], down)

        def cross(self, k):
            zz = (z2, zp, zm, z)[k]
            self.sx[k] = send(
                self.one_of(zz * 2 + 1 - xh, N1, 16), r2_x.at[k, :, :, self.cols], partner
            )

        def mid_up(self):
            self.a_up.wait_recv()
            add_both(self.cols, zp, 0, r1_low)
            self.b_up = send(self.both_of(zp, 0, N1), r1_up.at[:, :, :, self.cols], up)

        def mid_down(self):
            self.a_down.wait_recv()
            add_both(self.cols, zm, N1A, r1_high)
            self.b_down = send(self.both_of(zm, 0, N1), r1_down.at[:, :, :, self.cols], down)

        def crossed(self, k):
            self.sx[k].wait_recv()
            add_one(self.cols, (far, high, low, t)[k], N1, r2_x.at[k])
            if k == 0:
                cols = self.cols
                self.c_up = send(self.one_of(far, N1, N2A), r2_low.at[:, :, cols], up)
                self.c_down = send(self.one_of(far, N2A, 16), r2_high.at[:, :, cols], down)

        def third_up(self):
            self.c_up.wait_recv()
            add_one(self.cols, high, N1, r2_low)
            self.e_up = send(self.one_of(high, N1, 16), r2_up.at[:, :, self.cols], up)

        def third_down(self):
            self.c_down.wait_recv()
            add_one(self.cols, low, N2A, r2_high)
            self.e_down = send(self.one_of(low, N1, 16), r2_down.at[:, :, self.cols], down)

        def fold(self):
            cols = self.cols
            self.b_up.wait_recv()
            self.b_down.wait_recv()

            def step(i, carry):
                at = (there, i, slice(None), cols)
                total = partial[at].astype(F32) + r1_up[1 - xh, i, :, cols].astype(F32)
                partial[at] = (total + r1_down[1 - xh, i, :, cols].astype(F32)).astype(BF16)
                return carry

            lax.fori_loop(0, N1, step, 0, unroll=3)
            self.ex = send(self.one_of(there, 0, N1), r1_x.at[:, :, cols], partner)

        def finish_two(self):
            cols = self.cols
            self.e_up.wait_recv()
            self.e_down.wait_recv()

            def step(i, carry):
                at = (t, N1 + i, slice(None), cols)
                total = partial[at].astype(F32) + r2_up[i, :, cols].astype(F32)
                partial[at] = (total + r2_down[i, :, cols].astype(F32)).astype(BF16)
                return carry

            lax.fori_loop(0, 16 - N1, step, 0, unroll=True)

        def finish_one(self):
            cols = self.cols
            self.ex.wait_recv()

            def step(i, carry):
                at = (t, i, slice(None), cols)
                total = partial[at].astype(F32) + r1_up[xh, i, :, cols].astype(F32)
                total = total + r1_down[xh, i, :, cols].astype(F32)
                partial[at] = (total + r1_x[i, :, cols].astype(F32)).astype(BF16)
                return carry

            lax.fori_loop(0, N1, step, 0, unroll=3)

        def relay(self):
            cols = self.cols
            for k in range(16):
                device = dp_peer(k)[1]
                if k == 0:
                    landed[b, :, cols] = partial[t, chosen[k], :, cols]
                else:
                    staged[k, :, cols] = partial[t, chosen[k], :, cols]
                    self.copies.append(
                        send(staged.at[k, :, cols], landed.at[b, :, cols], device)
                    )

        def score(self):
            cols = self.cols
            weight = (final_gain[...] * score_weight[...]).reshape(1, D)[:, cols]
            position = lax.broadcasted_iota(jnp.int32, (16, D // 2), 0)
            for p in range(16):
                wanted = lengths[b * 16 + p] - 1 - t * 16
                row = jnp.where(position == wanted, partial[t, p, :, cols].astype(F32), 0.0)
                last_rows[p : p + 1] = jnp.sum(row, axis=0, keepdims=True)
            found = last_rows[...]
            sums = jnp.sum(found * found, axis=-1, keepdims=True)
            squares[self.h] = jnp.broadcast_to(sums, (16, 128))
            sums = jnp.sum(found * weight, axis=-1, keepdims=True)
            dots[self.h] = jnp.broadcast_to(sums, (16, 128))

    chosen = []
    for k in range(16):
        index = dp_peer(k)[0]
        pair = jnp.int32(0)
        for j in range(1, 16):
            pair = jnp.where(destination[b * 16 + j] == index, j, pair)
        chosen.append(pair)

    halves = (Half(0), Half(1))
    steps = {
        "b": Half.begin,
        "mu": Half.mid_up,
        "md": Half.mid_down,
        "tu": Half.third_up,
        "td": Half.third_down,
        "fo": Half.fold,
        "f2": Half.finish_two,
        "f1": Half.finish_one,
        "re": Half.relay,
        "sc": Half.score,
    }
    for k in range(4):
        steps[f"x{k}"] = functools.partial(Half.cross, k=k)
        steps[f"s{k}"] = functools.partial(Half.crossed, k=k)
    def begin_first():
        for name, h in ORDER[:EARLY]:
            steps[name](halves[h])

    block(far_x, between=begin_first)
    for name, h in ORDER[EARLY:]:
        steps[name](halves[h])

    mean = (squares[0] + squares[1]) / D
    score_one[...] = (dots[0] + dots[1]) * lax.rsqrt(mean + norm_eps)
    copies = [send(score_one, score_eight.at[t], tensor_peer(k)) for k in range(1, 8)]
    score_eight[t] = score_one[...]
    halves[1].relay()
    for copy in copies:
        copy.wait_recv()
    total = score_eight[0]
    for k in range(1, 8):
        total = total + score_eight[k]
    score_sum[...] = total
    score_all[b] = total
    copies = [send(score_sum, score_all.at[b], dp_peer(k)[1]) for k in range(1, 16)]
    writes = []

    def write(src, dst):
        copy = pltpu.make_async_copy(src, dst, local_sem.at[len(loads) + len(writes)])
        copy.start()
        writes.append(copy)

    for half in halves:
        for copy in half.copies:
            copy.wait_recv()
        write(landed.at[:, :, half.cols], relaid_out.at[:, :, half.cols])
    for copy in copies:
        copy.wait_recv()
    write(score_all, scores_out)
    send.drain()
    for copy in writes:
        copy.wait()


def any_spec():
    return pl.BlockSpec(memory_space=pl.ANY)


def vmem_spec():
    return pl.BlockSpec(memory_space=pltpu.VMEM)


def smem_spec():
    return pl.BlockSpec(memory_space=pltpu.SMEM)


def rotary_tables():
    index = np.arange(HEAD_DIM // 2, dtype=np.float32)
    frequency = np.power(np.float64(theta_base), -2.0 * index / HEAD_DIM).astype(np.float32)
    angles = np.arange(SEQ, dtype=np.float32)[:, None] * frequency[None, :]
    cosine, sine = np.cos(angles.astype(np.float64)), np.sin(angles.astype(np.float64))
    return (
        np.concatenate([cosine, cosine], axis=1).astype(np.float32),
        np.concatenate([-sine, sine], axis=1).astype(np.float32),
    )


def on_device(
    arrived, destination, query_of, lengths, attn_gain, q_weight, q_bias, k_weight, v_weight,
    v_bias, o_weight, mlp_gain, w_gate, w_up, w_down, final_gain, score_weight,
):
    cosine, sine = rotary_tables()
    pairs = lambda *lead: pltpu.VMEM((*lead, 16, D), BF16)
    relaid, scores = pl.pallas_call(
        layer_kernel,
        out_shape=[
            jax.ShapeDtypeStruct((16, 16, D), BF16),
            jax.ShapeDtypeStruct((16, 16, 128), F32),
        ],
        in_specs=[smem_spec()] * 2 + [vmem_spec()] * 2 + [any_spec()] * 14,
        out_specs=[any_spec()] * 2,
        scratch_shapes=[
            pltpu.VMEM((D,), F32),
            pltpu.VMEM((D,), F32),
            pltpu.VMEM((D,), F32),
            pltpu.VMEM((D,), F32),
            pltpu.VMEM((SEQ, HEAD_DIM), F32),
            pltpu.VMEM((SEQ, HEAD_DIM), F32),
            pltpu.VMEM((2, SEQ, D), BF16),
            pltpu.VMEM((D, KV_HEADS * HEAD_DIM), BF16),
            pltpu.VMEM((D, KV_HEADS * HEAD_DIM), BF16),
            pltpu.VMEM((D, HEADS * HEAD_DIM), BF16),
            pltpu.VMEM((HEADS * HEAD_DIM, D), BF16),
            pltpu.VMEM((8, HEAD_DIM), F32),
            pltpu.VMEM((8, 8, HEAD_DIM), F32),
            pltpu.VMEM((2 * SEQ, D), BF16),
            pltpu.VMEM((2 * SEQ, KV_HEADS * HEAD_DIM), BF16),
            pltpu.VMEM((2 * SEQ, KV_HEADS * HEAD_DIM), BF16),
            pltpu.VMEM((2 * SEQ, HEADS * HEAD_DIM), BF16),
            pltpu.VMEM((2 * SEQ, HEADS * HEAD_DIM), BF16),
            pltpu.VMEM((2 * SEQ, D), BF16),
            pltpu.VMEM((8, 2 * SEQ, D), BF16),
            pltpu.VMEM((FFL, D), BF16),
            pltpu.VMEM((FFL, D), BF16),
            pltpu.VMEM((FFP, D), BF16),
            pltpu.VMEM((256, D), BF16),
            pltpu.VMEM((2 * SEQ, FFP), BF16),
            pairs(8, 16),
            pairs(2, N1A),
            pairs(2, N1 - N1A),
            pairs(2, N1),
            pairs(2, N1),
            pairs(N1),
            pairs(4, 16 - N1),
            pairs(N2A - N1),
            pairs(16 - N2A),
            pairs(16 - N1),
            pairs(16 - N1),
            pairs(16),
            pairs(16),
            pltpu.VMEM((16, D // 2), F32),
            pltpu.VMEM((2, 16, 128), F32),
            pltpu.VMEM((2, 16, 128), F32),
            pltpu.VMEM((16, 128), F32),
            pltpu.VMEM((8, 16, 128), F32),
            pltpu.VMEM((16, 128), F32),
            pltpu.VMEM((16, 16, 128), F32),
            pltpu.SemaphoreType.DMA((19,)),
            pltpu.SemaphoreType.DMA((144,)),
            pltpu.SemaphoreType.DMA((144,)),
        ],
        compiler_params=pltpu.CompilerParams(
            collective_id=0, has_side_effects=True, vmem_limit_bytes=60 * 2**20
        ),
    )(
        lengths, destination, q_bias, v_bias, attn_gain, mlp_gain, final_gain, score_weight,
        cosine, sine, arrived, q_weight, k_weight, v_weight, o_weight, w_gate.T, w_up.T, w_down,
    )
    hidden_out = jnp.transpose(relaid, (1, 0, 2))

    group_index = lax.axis_index(DP)
    pair_score = scores[:, :, 0].reshape(-1)
    query_total = lax.axis_size(DP) * QUERY_DP
    membership = query_of[:, None] == jnp.arange(query_total, dtype=jnp.int32)[None, :]
    means = jnp.sum(jnp.where(membership, pair_score[:, None], 0.0), axis=0) / (
        pair_score.shape[0] // query_total
    )
    own_mean = jnp.sum(jnp.where(membership, means[None, :], 0.0), axis=1)
    here = (destination == group_index).reshape(16, 16)
    centred = jnp.sum(jnp.where(here, (pair_score - own_mean).reshape(16, 16), 0.0), axis=1)
    query_mean = lax.dynamic_slice_in_dim(means, group_index * QUERY_DP, QUERY_DP)
    return (hidden_out, centred, query_mean)


def solution(mesh):
    split = Mesh(mesh.devices.reshape(4, 2, 2, 4, 2), AXES)
    placed = (
        P(DP + TENSOR, None, None),
        P(),
        P(),
        P(),
        P(),
        P(None, TENSOR),
        P(TENSOR),
        P(),
        P(),
        P(),
        P(TENSOR, None),
        P(),
        P(None, TENSOR),
        P(None, TENSOR),
        P(TENSOR, None),
        P(),
        P(),
    )
    return jax.shard_map(
        on_device,
        mesh=split,
        in_specs=placed,
        out_specs=(P(TENSOR, DP, None), P(DP), P(DP)),
        check_vma=False,
    )
```

```python
import functools
import math

import jax
import jax.numpy as jnp
import numpy as np
from jax import lax
from jax.experimental import pallas as pl
from jax.experimental.pallas import tpu as pltpu
from jax.sharding import Mesh
from jax.sharding import PartitionSpec as P

AXES = ("y", "xl", "c", "z", "xh")
DP = ("y", "xl", "c")
TENSOR = ("z", "xh")
MESH = pl.DeviceIdType.MESH
F32 = jnp.float32
BF16 = jnp.bfloat16

KV_HEADS = 2
HEAD_DIM = 128
HEADS = 8
QUERY_DP = 2
theta_base = 1000000.0
norm_eps = 1e-06

SEQ = 128
D = 1536
FFL = 1120
FULL = 1024
TAIL = FFL - FULL
FFP = 1152

C1 = (0, 144)
C1A, C1B = (0, 80), (80, 144)
C2 = (144, 256)
C2A, C2B = (144, 208), (208, 256)
N1, N1A = 9, 5
N2A = 13


ORDER = (
    ("x2", 0), ("x3", 0), ("b", 0), ("x0", 0), ("x1", 0), ("x2", 1), ("b", 1), ("md", 0),
    ("mu", 0), ("s0", 0), ("x1", 1), ("md", 1), ("x0", 1), ("mu", 1), ("fo", 0), ("s0", 1),
    ("s2", 1), ("s1", 0), ("s3", 0), ("tu", 0), ("s2", 0), ("td", 0), ("x3", 1), ("s1", 1),
    ("td", 1), ("fo", 1), ("tu", 1), ("s3", 1), ("f1", 0), ("f2", 0), ("re", 0), ("sc", 0),
    ("f1", 1), ("f2", 1), ("sc", 1),
)


EARLY = 5


def z_at(step):
    return lax.rem(lax.axis_index("z") + step + 4, 4)


class Sender:
    def __init__(self, send_sem, recv_sem):
        self.send_sem, self.recv_sem, self.count = send_sem, recv_sem, 0
        self.open = []

    def __call__(self, src, dst, device):
        i = self.count
        self.count += 1
        copy = pltpu.make_async_remote_copy(
            src_ref=src,
            dst_ref=dst,
            send_sem=self.send_sem.at[i],
            recv_sem=self.recv_sem.at[i],
            device_id=device,
            device_id_type=MESH,
        )
        copy.start()
        self.open.append(copy)
        return copy

    def drain(self):
        for copy in self.open:
            copy.wait_send()
        self.open = []


def tensor_peer(k):
    index = lax.rem(lax.axis_index("z") * 2 + lax.axis_index("xh") + k, 8)
    return {"z": index // 2, "xh": lax.rem(index, 2)}


def dp_peer(k):
    index = lax.axis_index("y") * 4 + lax.axis_index("xl") * 2 + lax.axis_index("c")
    index = lax.rem(index + k, 16)
    return index, {"y": index // 4, "xl": lax.rem(index // 2, 2), "c": lax.rem(index, 2)}


def rms_rows(values, gain):
    scale = lax.rsqrt(jnp.mean(values * values, axis=-1, keepdims=True) + norm_eps)
    return values * scale * gain


def rotate(values, cosine, sine):
    return values * cosine + pltpu.roll(values, HEAD_DIM // 2, 1) * sine


def layer_kernel(
    lengths, destination, q_bias, v_bias,
    gain_in, mlp_gain_in, final_gain_in, score_weight_in, cosine_in, sine_in,
    arrived, q_w, k_w, v_w, o_w, w_gate, w_up, w_down,
    relaid_out, scores_out,
    gain, mlp_gain, final_gain, score_weight, cosine, sine,
    x_v, k_v, v_v, q_all, o_all, bias_one, bias_all, normed, keys, values, queries, context,
    after_v, gathered, wg, wu, wd, w_tail, active, partial,
    r1_low, r1_high, r1_up, r1_down, r1_x, r2_x, r2_low, r2_high, r2_up, r2_down,
    staged, landed, last_rows, squares, dots, score_one, score_eight, score_sum, score_all,
    local_sem, send_sem, recv_sem,
):
    z, xh, c = lax.axis_index("z"), lax.axis_index("xh"), lax.axis_index("c")
    y, xl = lax.axis_index("y"), lax.axis_index("xl")
    t = z * 2 + xh
    b = y * 4 + xl * 2 + c
    partner, sibling = {"xh": 1 - xh}, {"c": 1 - c}
    up, down = {"z": z_at(1)}, {"z": z_at(-1)}
    zp, zm, z2 = z_at(1), z_at(-1), z_at(2)
    here, there = t, z * 2 + 1 - xh
    low, high = zm * 2 + xh, zp * 2 + xh
    low_x, high_x = zm * 2 + 1 - xh, zp * 2 + 1 - xh
    far, far_x = z2 * 2 + xh, z2 * 2 + 1 - xh

    def q_cols(index):
        return pl.ds(pl.multiple_of(index * HEAD_DIM, HEAD_DIM), HEAD_DIM)

    sources = [
        (arrived, x_v),
        (k_w, k_v),
        (v_w, v_v),
        (q_w, q_all.at[:, q_cols(t)]),
        (o_w, o_all.at[pl.ds(pl.multiple_of(t * HEAD_DIM, HEAD_DIM), HEAD_DIM)]),
        (w_gate, wg),
        (w_up, wu),
        (w_down, wd.at[pl.ds(0, FFL)]),
        (w_gate.at[pl.ds(FULL, TAIL)], w_tail.at[pl.ds(0, TAIL)]),
        (w_up.at[pl.ds(FULL, TAIL)], w_tail.at[pl.ds(128, TAIL)]),
        (gain_in, gain),
        (cosine_in, cosine),
        (sine_in, sine),
        (mlp_gain_in, mlp_gain),
        (final_gain_in, final_gain),
        (score_weight_in, score_weight),
    ]
    loads = [
        pltpu.make_async_copy(src, dst, local_sem.at[i]) for i, (src, dst) in enumerate(sources)
    ]
    peers = [tensor_peer(k) for k in range(1, 8)] + [dp_peer(k)[1] for k in range(1, 16)]
    barrier = pltpu.get_barrier_semaphore()
    for device in peers:
        pl.semaphore_signal(barrier, inc=1, device_id=device, device_id_type=MESH)
    for i in (3, 4, 0, 1, 2, *range(10, 16)):
        loads[i].start()
    bias_one[...] = jnp.broadcast_to(q_bias[...].reshape(1, HEAD_DIM).astype(F32), bias_one.shape)
    pl.semaphore_wait(barrier, len(peers))
    send = Sender(send_sem, recv_sem)

    half_q, half_o = D // 2, HEAD_DIM // 2

    def q_piece(index, sub=None):
        size = half_q if sub is None else half_q // 2
        start = c * half_q + (0 if sub is None else sub * size)
        return q_all.at[pl.ds(pl.multiple_of(start, 128), size), q_cols(index)]

    parity = lax.rem(y, 2)

    def o_rows(index, side, sub):
        size = half_o // 2 if sub is None else half_o // 4
        start = index * HEAD_DIM + c * half_o + side * (half_o // 2)
        start = start + (0 if sub is None else sub * size)
        return o_all.at[pl.ds(pl.multiple_of(start, 16), size)]

    def o_piece(index, sub=None):
        return o_rows(index, parity, sub)

    def o_other(index, sub):
        return o_rows(index, 1 - parity, sub)

    own_q, own_o = q_piece(t), o_piece(t)
    loads[3].wait()
    loads[4].wait()

    o_u, o_d = send(own_o, o_piece(t), up), send(own_o, o_piece(t), down)
    q_x = send(own_q, q_piece(t), partner)
    q_u, q_d = send(own_q, q_piece(t), up), send(own_q, q_piece(t), down)
    bias_copies = [send(bias_one, bias_all.at[t], tensor_peer(k)) for k in range(1, 8)]
    o_x = send(own_o, o_piece(t), partner)
    for load in loads[5:10]:
        load.start()

    loads[0].wait()
    for load in loads[10:]:
        load.wait()
    x = x_v[...].reshape(2 * SEQ, D)
    normed[...] = rms_rows(x.astype(F32), gain[...].reshape(1, D)).astype(BF16)
    loads[1].wait()
    loads[2].wait()
    cos_rows = jnp.concatenate([cosine[...]] * 2, axis=0)
    sin_rows = jnp.concatenate([sine[...]] * 2, axis=0)
    k_f = jnp.dot(normed[...], k_v[...], preferred_element_type=F32)
    for g in range(KV_HEADS):
        cols = slice(g * HEAD_DIM, (g + 1) * HEAD_DIM)
        keys[:, cols] = rotate(k_f[:, cols], cos_rows, sin_rows).astype(BF16)
    v_f = jnp.dot(normed[...], v_v[...], preferred_element_type=F32)
    values[...] = (v_f + v_bias[...].reshape(1, -1).astype(F32)).astype(BF16)

    q_sib, o_sib = [], []

    def project_q(i):
        cols = pl.ds(pl.multiple_of(i * 256, 256), 256)
        q_f = jnp.dot(normed[...], q_all[:, cols], preferred_element_type=F32)
        for e in range(2):
            q_e = q_f[:, e * HEAD_DIM : (e + 1) * HEAD_DIM] + bias_all[2 * i + e][0:1]
            at = pl.ds(pl.multiple_of(i * 256 + e * HEAD_DIM, HEAD_DIM), HEAD_DIM)
            queries[:, at] = rotate(q_e, cos_rows, sin_rows).astype(BF16)

    def share(piece, index, sub, copies):
        copies.append(send(piece(index, sub), piece(index, sub), sibling))

    def pass_piece(piece, index, sub, device):
        return send(piece(index, sub), piece(index, sub), device)

    y_ahead = {"y": lax.rem(y + 1, 4)}
    y_back = {"y": lax.rem(y + 3, 4)}
    over_y = []

    def spread(index, sub=None):
        share(o_piece, index, sub, o_sib)
        for part, device in ((0, y_ahead), (1, y_back)):
            if sub is None or sub == part:
                piece = o_piece(index, part)
                over_y.append((send(piece, piece, device), index, part))

    def collect(count):
        for _ in range(count):
            copy, index, part = over_y.pop(0)
            copy.wait_recv()
            share(o_other, index, part, o_sib)

    o_u.wait_recv()
    o_fu = pass_piece(o_piece, low, 0, up)
    o_xl = pass_piece(o_piece, low, None, partner)
    spread(low)
    o_d.wait_recv()
    o_fd = pass_piece(o_piece, high, 1, down)
    o_xh = pass_piece(o_piece, high, None, partner)
    spread(high)
    q_x.wait_recv()
    q_xu = pass_piece(q_piece, there, None, up)
    q_xd = pass_piece(q_piece, there, None, down)
    share(q_piece, there, None, q_sib)
    q_u.wait_recv()
    q_fu = pass_piece(q_piece, low, 0, up)
    share(q_piece, low, None, q_sib)
    q_d.wait_recv()
    q_fd = pass_piece(q_piece, high, 1, down)
    share(q_piece, high, None, q_sib)
    collect(4)
    o_x.wait_recv()
    spread(there)
    o_fu.wait_recv()
    o_xfa = pass_piece(o_piece, far, 0, partner)
    spread(far, 0)
    o_fd.wait_recv()
    o_xfb = pass_piece(o_piece, far, 1, partner)
    spread(far, 1)
    for copy in bias_copies:
        copy.wait_recv()
    bias_all[t] = bias_one[...]
    q_sib[0].wait_recv()
    project_q(z)
    o_xl.wait_recv()
    spread(low_x)
    collect(4)
    q_xu.wait_recv()
    q_fxu = pass_piece(q_piece, low_x, 0, up)
    share(q_piece, low_x, None, q_sib)
    q_xd.wait_recv()
    q_fxd = pass_piece(q_piece, high_x, 1, down)
    share(q_piece, high_x, None, q_sib)
    o_xh.wait_recv()
    spread(high_x)
    collect(2)
    q_fu.wait_recv()
    share(q_piece, far, 0, q_sib)
    q_fd.wait_recv()
    share(q_piece, far, 1, q_sib)
    for copy in q_sib[1:5]:
        copy.wait_recv()
    project_q(zm)
    project_q(zp)
    o_xfa.wait_recv()
    spread(far_x, 0)
    o_xfb.wait_recv()
    spread(far_x, 1)
    collect(2)
    q_fxu.wait_recv()
    share(q_piece, far_x, 0, q_sib)
    q_fxd.wait_recv()
    share(q_piece, far_x, 1, q_sib)
    collect(2)
    for copy in q_sib[5:]:
        copy.wait_recv()
    project_q(z2)

    q_pos = lax.broadcasted_iota(jnp.int32, (SEQ, SEQ), 0)
    k_pos = lax.broadcasted_iota(jnp.int32, (SEQ, SEQ), 1)
    group = HEADS // KV_HEADS
    first_pair = (b * 8 + t) * 2
    for copy in o_sib:
        copy.wait_recv()

    def attend(p):
        rows = slice(p * SEQ, (p + 1) * SEQ)
        allowed = (k_pos <= q_pos) & (k_pos < lengths[first_pair + p])
        allowed = jnp.concatenate([allowed.astype(F32)] * group, axis=0) > 0.5
        for g in range(KV_HEADS):
            cols = slice(g * HEAD_DIM, (g + 1) * HEAD_DIM)
            q_g = jnp.concatenate(
                [
                    queries[rows, (g * group + h) * HEAD_DIM : (g * group + h + 1) * HEAD_DIM]
                    for h in range(group)
                ],
                axis=0,
            )
            logits = lax.dot_general(
                q_g, keys[rows, cols], (((1,), (1,)), ((), ())), preferred_element_type=F32
            ) / math.sqrt(HEAD_DIM)
            logits = jnp.where(allowed, logits, -1e30)
            shifted = jnp.exp(logits - jnp.max(logits, axis=-1, keepdims=True))
            probs = (shifted / jnp.sum(shifted, axis=-1, keepdims=True)).astype(BF16)
            ctx = jnp.dot(probs, values[rows, cols], preferred_element_type=F32).astype(BF16)
            for h in range(group):
                at = (g * group + h) * HEAD_DIM
                context[rows, at : at + HEAD_DIM] = ctx[h * SEQ : (h + 1) * SEQ]
        for i in range(D // 256):
            cols = slice(i * 256, (i + 1) * 256)
            attended = jnp.dot(context[rows], o_all[:, cols], preferred_element_type=F32)
            after_v[rows, cols] = (x_v[p, :, cols].astype(F32) + attended).astype(BF16)
        after_rows = after_v[rows].astype(F32)
        gathered[t, rows] = rms_rows(after_rows, mlp_gain[...].reshape(1, D)).astype(BF16)

    def block_rows(g, span):
        return gathered.at[g, pl.ds(span[0], span[1] - span[0])]

    def pass_on(g, span, device):
        return send(block_rows(g, span), block_rows(g, span), device)

    attend(1)
    u2 = pass_on(here, C2, up)
    d2 = pass_on(here, C2, down)
    x2 = pass_on(here, C2, partner)
    attend(0)
    u1 = pass_on(here, C1, up)
    d1 = pass_on(here, C1, down)
    x1 = pass_on(here, C1, partner)

    for load in loads[5:10]:
        load.wait()
    wd[FFL:FFP] = jnp.zeros((FFP - FFL, D), BF16)
    w_tail[TAIL:128] = jnp.zeros((128 - TAIL, D), BF16)
    w_tail[128 + TAIL :] = jnp.zeros((128 - TAIL, D), BF16)

    def gated(gate_values, up_values):
        return (gate_values / (1.0 + jnp.exp(-gate_values)) * up_values).astype(BF16)

    def by_rows(g, weights):
        return lax.dot_general(
            gathered[g], weights, (((1,), (1,)), ((), ())), preferred_element_type=F32
        )

    def block(g, own=False, between=None):
        def hidden(i, carry):
            at = pl.ds(pl.multiple_of(i * 256, 256), 256)
            active[:, at] = gated(by_rows(g, wg[at]), by_rows(g, wu[at]))
            return carry

        lax.fori_loop(0, FULL // 256, hidden, 0, unroll=True)
        both = by_rows(g, w_tail[...])
        active[:, FULL:FFP] = gated(both[:, :128], both[:, 128:])

        for i in range(D // 256):
            if i == D // 512 and between is not None:
                between()
            cols = slice(i * 256, (i + 1) * 256)
            result = jnp.dot(active[...], wd[:, cols], preferred_element_type=F32)
            if own:
                result = result.astype(BF16).astype(F32) + after_v[:, cols].astype(F32)
            result = result.astype(BF16).reshape(2, 8, 16, 256)
            for owner in range(8):
                partial[owner, pl.ds(2 * g, 2), :, cols] = result[:, owner]

    block(here, own=True)
    u2.wait_recv()
    f2u = pass_on(low, C2A, up)
    x_low = pass_on(low, C2, partner)
    d2.wait_recv()
    f2d = pass_on(high, C2B, down)
    x_high = pass_on(high, C2, partner)
    x1.wait_recv()
    xu = pass_on(there, C1, up)
    xd = pass_on(there, C1, down)
    u1.wait_recv()
    f1u = pass_on(low, C1A, up)
    d1.wait_recv()
    f1d = pass_on(high, C1B, down)
    block(low)
    f2u.wait_recv()
    x_far_a = pass_on(far, C2A, partner)
    f2d.wait_recv()
    x_far_b = pass_on(far, C2B, partner)
    block(high)
    x2.wait_recv()
    block(there)
    xu.wait_recv()
    fxu = pass_on(low_x, C1A, up)
    xd.wait_recv()
    fxd = pass_on(high_x, C1B, down)
    x_low.wait_recv()
    block(low_x)
    x_high.wait_recv()
    block(high_x)
    f1u.wait_recv()
    f1d.wait_recv()
    block(far)
    fxu.wait_recv()
    fxd.wait_recv()
    x_far_a.wait_recv()
    x_far_b.wait_recv()

    def add_both(cols, zz, lo, extra):
        def step(i, carry):
            for e in range(2):
                at = (2 * zz + e, lo + i, slice(None), cols)
                partial[at] = (
                    partial[at].astype(F32) + extra[e, i, :, cols].astype(F32)
                ).astype(BF16)
            return carry

        lax.fori_loop(0, extra.shape[1], step, 0, unroll=True)

    def add_one(cols, index, lo, extra):
        def step(i, carry):
            at = (index, lo + i, slice(None), cols)
            partial[at] = (partial[at].astype(F32) + extra[i, :, cols].astype(F32)).astype(BF16)
            return carry

        lax.fori_loop(0, extra.shape[0], step, 0, unroll=True)

    class Half:
        def __init__(self, h):
            self.h, self.sx, self.copies = h, [None] * 4, []
            self.cols = slice(h * (D // 2), (h + 1) * (D // 2))

        def both_of(self, zz, lo, hi):
            return partial.at[pl.ds(2 * zz, 2), pl.ds(lo, hi - lo), :, self.cols]

        def one_of(self, index, lo, hi):
            return partial.at[index, pl.ds(lo, hi - lo), :, self.cols]

        def begin(self):
            cols = self.cols
            self.a_up = send(self.both_of(z2, 0, N1A), r1_low.at[:, :, :, cols], up)
            self.a_down = send(self.both_of(z2, N1A, N1), r1_high.at[:, :, :, cols], down)

        def cross(self, k):
            zz = (z2, zp, zm, z)[k]
            self.sx[k] = send(
                self.one_of(zz * 2 + 1 - xh, N1, 16), r2_x.at[k, :, :, self.cols], partner
            )

        def mid_up(self):
            self.a_up.wait_recv()
            add_both(self.cols, zp, 0, r1_low)
            self.b_up = send(self.both_of(zp, 0, N1), r1_up.at[:, :, :, self.cols], up)

        def mid_down(self):
            self.a_down.wait_recv()
            add_both(self.cols, zm, N1A, r1_high)
            self.b_down = send(self.both_of(zm, 0, N1), r1_down.at[:, :, :, self.cols], down)

        def crossed(self, k):
            self.sx[k].wait_recv()
            add_one(self.cols, (far, high, low, t)[k], N1, r2_x.at[k])
            if k == 0:
                cols = self.cols
                self.c_up = send(self.one_of(far, N1, N2A), r2_low.at[:, :, cols], up)
                self.c_down = send(self.one_of(far, N2A, 16), r2_high.at[:, :, cols], down)

        def third_up(self):
            self.c_up.wait_recv()
            add_one(self.cols, high, N1, r2_low)
            self.e_up = send(self.one_of(high, N1, 16), r2_up.at[:, :, self.cols], up)

        def third_down(self):
            self.c_down.wait_recv()
            add_one(self.cols, low, N2A, r2_high)
            self.e_down = send(self.one_of(low, N1, 16), r2_down.at[:, :, self.cols], down)

        def fold(self):
            cols = self.cols
            self.b_up.wait_recv()
            self.b_down.wait_recv()

            def step(i, carry):
                at = (there, i, slice(None), cols)
                total = partial[at].astype(F32) + r1_up[1 - xh, i, :, cols].astype(F32)
                partial[at] = (total + r1_down[1 - xh, i, :, cols].astype(F32)).astype(BF16)
                return carry

            lax.fori_loop(0, N1, step, 0, unroll=3)
            self.ex = send(self.one_of(there, 0, N1), r1_x.at[:, :, cols], partner)

        def finish_two(self):
            cols = self.cols
            self.e_up.wait_recv()
            self.e_down.wait_recv()

            def step(i, carry):
                at = (t, N1 + i, slice(None), cols)
                total = partial[at].astype(F32) + r2_up[i, :, cols].astype(F32)
                partial[at] = (total + r2_down[i, :, cols].astype(F32)).astype(BF16)
                return carry

            lax.fori_loop(0, 16 - N1, step, 0, unroll=True)

        def finish_one(self):
            cols = self.cols
            self.ex.wait_recv()

            def step(i, carry):
                at = (t, i, slice(None), cols)
                total = partial[at].astype(F32) + r1_up[xh, i, :, cols].astype(F32)
                total = total + r1_down[xh, i, :, cols].astype(F32)
                partial[at] = (total + r1_x[i, :, cols].astype(F32)).astype(BF16)
                return carry

            lax.fori_loop(0, N1, step, 0, unroll=3)

        def relay(self):
            cols = self.cols
            for k in range(16):
                device = dp_peer(k)[1]
                if k == 0:
                    landed[b, :, cols] = partial[t, chosen[k], :, cols]
                else:
                    staged[k, :, cols] = partial[t, chosen[k], :, cols]
                    self.copies.append(
                        send(staged.at[k, :, cols], landed.at[b, :, cols], device)
                    )

        def score(self):
            cols = self.cols
            weight = (final_gain[...] * score_weight[...]).reshape(1, D)[:, cols]
            position = lax.broadcasted_iota(jnp.int32, (16, D // 2), 0)
            for p in range(16):
                wanted = lengths[b * 16 + p] - 1 - t * 16
                row = jnp.where(position == wanted, partial[t, p, :, cols].astype(F32), 0.0)
                last_rows[p : p + 1] = jnp.sum(row, axis=0, keepdims=True)
            found = last_rows[...]
            sums = jnp.sum(found * found, axis=-1, keepdims=True)
            squares[self.h] = jnp.broadcast_to(sums, (16, 128))
            sums = jnp.sum(found * weight, axis=-1, keepdims=True)
            dots[self.h] = jnp.broadcast_to(sums, (16, 128))

    chosen = []
    for k in range(16):
        index = dp_peer(k)[0]
        pair = jnp.int32(0)
        for j in range(1, 16):
            pair = jnp.where(destination[b * 16 + j] == index, j, pair)
        chosen.append(pair)

    halves = (Half(0), Half(1))
    steps = {
        "b": Half.begin,
        "mu": Half.mid_up,
        "md": Half.mid_down,
        "tu": Half.third_up,
        "td": Half.third_down,
        "fo": Half.fold,
        "f2": Half.finish_two,
        "f1": Half.finish_one,
        "re": Half.relay,
        "sc": Half.score,
    }
    for k in range(4):
        steps[f"x{k}"] = functools.partial(Half.cross, k=k)
        steps[f"s{k}"] = functools.partial(Half.crossed, k=k)
    def begin_first():
        for name, h in ORDER[:EARLY]:
            steps[name](halves[h])

    block(far_x, between=begin_first)
    for name, h in ORDER[EARLY:]:
        steps[name](halves[h])

    mean = (squares[0] + squares[1]) / D
    score_one[...] = (dots[0] + dots[1]) * lax.rsqrt(mean + norm_eps)
    copies = [send(score_one, score_eight.at[t], tensor_peer(k)) for k in range(1, 8)]
    score_eight[t] = score_one[...]
    halves[1].relay()
    for copy in copies:
        copy.wait_recv()
    total = score_eight[0]
    for k in range(1, 8):
        total = total + score_eight[k]
    score_sum[...] = total
    score_all[b] = total
    copies = [send(score_sum, score_all.at[b], dp_peer(k)[1]) for k in range(1, 16)]
    writes = []

    def write(src, dst):
        copy = pltpu.make_async_copy(src, dst, local_sem.at[len(loads) + len(writes)])
        copy.start()
        writes.append(copy)

    for half in halves:
        for copy in half.copies:
            copy.wait_recv()
        write(landed.at[:, :, half.cols], relaid_out.at[:, :, half.cols])
    for copy in copies:
        copy.wait_recv()
    write(score_all, scores_out)
    send.drain()
    for copy in writes:
        copy.wait()


def any_spec():
    return pl.BlockSpec(memory_space=pl.ANY)


def vmem_spec():
    return pl.BlockSpec(memory_space=pltpu.VMEM)


def smem_spec():
    return pl.BlockSpec(memory_space=pltpu.SMEM)


def rotary_tables():
    index = np.arange(HEAD_DIM // 2, dtype=np.float32)
    frequency = np.power(np.float64(theta_base), -2.0 * index / HEAD_DIM).astype(np.float32)
    angles = np.arange(SEQ, dtype=np.float32)[:, None] * frequency[None, :]
    cosine, sine = np.cos(angles.astype(np.float64)), np.sin(angles.astype(np.float64))
    return (
        np.concatenate([cosine, cosine], axis=1).astype(np.float32),
        np.concatenate([-sine, sine], axis=1).astype(np.float32),
    )


def on_device(
    arrived, destination, query_of, lengths, attn_gain, q_weight, q_bias, k_weight, v_weight,
    v_bias, o_weight, mlp_gain, w_gate, w_up, w_down, final_gain, score_weight,
):
    cosine, sine = rotary_tables()
    pairs = lambda *lead: pltpu.VMEM((*lead, 16, D), BF16)
    relaid, scores = pl.pallas_call(
        layer_kernel,
        out_shape=[
            jax.ShapeDtypeStruct((16, 16, D), BF16),
            jax.ShapeDtypeStruct((16, 16, 128), F32),
        ],
        in_specs=[smem_spec()] * 2 + [vmem_spec()] * 2 + [any_spec()] * 14,
        out_specs=[any_spec()] * 2,
        scratch_shapes=[
            pltpu.VMEM((D,), F32),
            pltpu.VMEM((D,), F32),
            pltpu.VMEM((D,), F32),
            pltpu.VMEM((D,), F32),
            pltpu.VMEM((SEQ, HEAD_DIM), F32),
            pltpu.VMEM((SEQ, HEAD_DIM), F32),
            pltpu.VMEM((2, SEQ, D), BF16),
            pltpu.VMEM((D, KV_HEADS * HEAD_DIM), BF16),
            pltpu.VMEM((D, KV_HEADS * HEAD_DIM), BF16),
            pltpu.VMEM((D, HEADS * HEAD_DIM), BF16),
            pltpu.VMEM((HEADS * HEAD_DIM, D), BF16),
            pltpu.VMEM((8, HEAD_DIM), F32),
            pltpu.VMEM((8, 8, HEAD_DIM), F32),
            pltpu.VMEM((2 * SEQ, D), BF16),
            pltpu.VMEM((2 * SEQ, KV_HEADS * HEAD_DIM), BF16),
            pltpu.VMEM((2 * SEQ, KV_HEADS * HEAD_DIM), BF16),
            pltpu.VMEM((2 * SEQ, HEADS * HEAD_DIM), BF16),
            pltpu.VMEM((2 * SEQ, HEADS * HEAD_DIM), BF16),
            pltpu.VMEM((2 * SEQ, D), BF16),
            pltpu.VMEM((8, 2 * SEQ, D), BF16),
            pltpu.VMEM((FFL, D), BF16),
            pltpu.VMEM((FFL, D), BF16),
            pltpu.VMEM((FFP, D), BF16),
            pltpu.VMEM((256, D), BF16),
            pltpu.VMEM((2 * SEQ, FFP), BF16),
            pairs(8, 16),
            pairs(2, N1A),
            pairs(2, N1 - N1A),
            pairs(2, N1),
            pairs(2, N1),
            pairs(N1),
            pairs(4, 16 - N1),
            pairs(N2A - N1),
            pairs(16 - N2A),
            pairs(16 - N1),
            pairs(16 - N1),
            pairs(16),
            pairs(16),
            pltpu.VMEM((16, D // 2), F32),
            pltpu.VMEM((2, 16, 128), F32),
            pltpu.VMEM((2, 16, 128), F32),
            pltpu.VMEM((16, 128), F32),
            pltpu.VMEM((8, 16, 128), F32),
            pltpu.VMEM((16, 128), F32),
            pltpu.VMEM((16, 16, 128), F32),
            pltpu.SemaphoreType.DMA((19,)),
            pltpu.SemaphoreType.DMA((176,)),
            pltpu.SemaphoreType.DMA((176,)),
        ],
        compiler_params=pltpu.CompilerParams(
            collective_id=0, has_side_effects=True, vmem_limit_bytes=60 * 2**20
        ),
    )(
        lengths, destination, q_bias, v_bias, attn_gain, mlp_gain, final_gain, score_weight,
        cosine, sine, arrived, q_weight, k_weight, v_weight, o_weight, w_gate.T, w_up.T, w_down,
    )
    hidden_out = jnp.transpose(relaid, (1, 0, 2))

    group_index = lax.axis_index(DP)
    pair_score = scores[:, :, 0].reshape(-1)
    query_total = lax.axis_size(DP) * QUERY_DP
    membership = query_of[:, None] == jnp.arange(query_total, dtype=jnp.int32)[None, :]
    means = jnp.sum(jnp.where(membership, pair_score[:, None], 0.0), axis=0) / (
        pair_score.shape[0] // query_total
    )
    own_mean = jnp.sum(jnp.where(membership, means[None, :], 0.0), axis=1)
    here = (destination == group_index).reshape(16, 16)
    centred = jnp.sum(jnp.where(here, (pair_score - own_mean).reshape(16, 16), 0.0), axis=1)
    query_mean = lax.dynamic_slice_in_dim(means, group_index * QUERY_DP, QUERY_DP)
    return (hidden_out, centred, query_mean)


def solution(mesh):
    split = Mesh(mesh.devices.reshape(4, 2, 2, 4, 2), AXES)
    placed = (
        P(DP + TENSOR, None, None),
        P(),
        P(),
        P(),
        P(),
        P(None, TENSOR),
        P(TENSOR),
        P(),
        P(),
        P(),
        P(TENSOR, None),
        P(),
        P(None, TENSOR),
        P(None, TENSOR),
        P(TENSOR, None),
        P(),
        P(),
    )
    return jax.shard_map(
        on_device,
        mesh=split,
        in_specs=placed,
        out_specs=(P(TENSOR, DP, None), P(DP), P(DP)),
        check_vma=False,
    )
```

```python
import functools
import math

import jax
import jax.numpy as jnp
import numpy as np
from jax import lax
from jax.experimental import pallas as pl
from jax.experimental.pallas import tpu as pltpu
from jax.sharding import Mesh
from jax.sharding import PartitionSpec as P

AXES = ("y", "xl", "c", "z", "xh")
DP = ("y", "xl", "c")
TENSOR = ("z", "xh")
MESH = pl.DeviceIdType.MESH
F32 = jnp.float32
BF16 = jnp.bfloat16

KV_HEADS = 2
HEAD_DIM = 128
HEADS = 8
QUERY_DP = 2
PER_QUERY = 8
theta_base = 1000000.0
norm_eps = 1e-06

SEQ = 128
D = 1536
FFL = 1120
FULL = 1024
TAIL = FFL - FULL
FFP = 1152

C1 = (0, 144)
C1A, C1B = (0, 80), (80, 144)
C2 = (144, 256)
C2A, C2B = (144, 208), (208, 256)
N1, N1A = 9, 5
N2A = 13


ORDER = (
    ("x2", 0), ("x3", 0), ("b", 0), ("x0", 0), ("x1", 0), ("x2", 1), ("b", 1), ("md", 0),
    ("mu", 0), ("s0", 0), ("x1", 1), ("md", 1), ("x0", 1), ("mu", 1), ("fo", 0), ("s0", 1),
    ("s2", 1), ("s1", 0), ("s3", 0), ("tu", 0), ("s2", 0), ("td", 0), ("x3", 1), ("s1", 1),
    ("td", 1), ("fo", 1), ("tu", 1), ("s3", 1), ("f1", 0), ("f2", 0), ("re", 0), ("sc", 0),
    ("f1", 1), ("f2", 1), ("sc", 1),
)


EARLY = 5


def z_at(step):
    return lax.rem(lax.axis_index("z") + step + 4, 4)


class Sender:
    def __init__(self, send_sem, recv_sem):
        self.send_sem, self.recv_sem, self.count = send_sem, recv_sem, 0
        self.open = []

    def __call__(self, src, dst, device):
        i = self.count
        self.count += 1
        copy = pltpu.make_async_remote_copy(
            src_ref=src,
            dst_ref=dst,
            send_sem=self.send_sem.at[i],
            recv_sem=self.recv_sem.at[i],
            device_id=device,
            device_id_type=MESH,
        )
        copy.start()
        self.open.append(copy)
        return copy

    def drain(self):
        for copy in self.open:
            copy.wait_send()
        self.open = []


def tensor_peer(k):
    index = lax.rem(lax.axis_index("z") * 2 + lax.axis_index("xh") + k, 8)
    return {"z": index // 2, "xh": lax.rem(index, 2)}


def dp_peer(k):
    index = lax.axis_index("y") * 4 + lax.axis_index("xl") * 2 + lax.axis_index("c")
    index = lax.rem(index + k, 16)
    return index, {"y": index // 4, "xl": lax.rem(index // 2, 2), "c": lax.rem(index, 2)}


def rms_rows(values, gain):
    scale = lax.rsqrt(jnp.mean(values * values, axis=-1, keepdims=True) + norm_eps)
    return values * scale * gain


def rotate(values, cosine, sine):
    return values * cosine + pltpu.roll(values, HEAD_DIM // 2, 1) * sine


def layer_kernel(
    lengths, destination, query_of, q_bias, v_bias,
    gain_in, mlp_gain_in, final_gain_in, score_weight_in, cosine_in, sine_in,
    arrived, q_w, k_w, v_w, o_w, w_gate, w_up, w_down,
    relaid_out, centred_out, mean_out,
    gain, mlp_gain, final_gain, score_weight, cosine, sine,
    x_v, k_v, v_v, q_all, o_all, bias_one, bias_all, normed, keys, values, queries, context,
    after_v, gathered, wg, wu, wd, w_tail, active, partial,
    r1_low, r1_high, r1_up, r1_down, r1_x, r2_x, r2_low, r2_high, r2_up, r2_down,
    staged, landed, last_rows, squares, dots, score_one, score_eight, score_sum, score_all,
    query_rows, target_rows,
    local_sem, send_sem, recv_sem,
):
    z, xh, c = lax.axis_index("z"), lax.axis_index("xh"), lax.axis_index("c")
    y, xl = lax.axis_index("y"), lax.axis_index("xl")
    t = z * 2 + xh
    b = y * 4 + xl * 2 + c
    partner, sibling = {"xh": 1 - xh}, {"c": 1 - c}
    up, down = {"z": z_at(1)}, {"z": z_at(-1)}
    zp, zm, z2 = z_at(1), z_at(-1), z_at(2)
    here, there = t, z * 2 + 1 - xh
    low, high = zm * 2 + xh, zp * 2 + xh
    low_x, high_x = zm * 2 + 1 - xh, zp * 2 + 1 - xh
    far, far_x = z2 * 2 + xh, z2 * 2 + 1 - xh

    def q_cols(index):
        return pl.ds(pl.multiple_of(index * HEAD_DIM, HEAD_DIM), HEAD_DIM)

    sources = [
        (arrived, x_v),
        (k_w, k_v),
        (v_w, v_v),
        (q_w, q_all.at[:, q_cols(t)]),
        (o_w, o_all.at[pl.ds(pl.multiple_of(t * HEAD_DIM, HEAD_DIM), HEAD_DIM)]),
        (w_gate, wg),
        (w_up, wu),
        (w_down, wd.at[pl.ds(0, FFL)]),
        (w_gate.at[pl.ds(FULL, TAIL)], w_tail.at[pl.ds(0, TAIL)]),
        (w_up.at[pl.ds(FULL, TAIL)], w_tail.at[pl.ds(128, TAIL)]),
        (gain_in, gain),
        (cosine_in, cosine),
        (sine_in, sine),
        (mlp_gain_in, mlp_gain),
        (final_gain_in, final_gain),
        (score_weight_in, score_weight),
    ]
    loads = [
        pltpu.make_async_copy(src, dst, local_sem.at[i]) for i, (src, dst) in enumerate(sources)
    ]
    peers = [tensor_peer(k) for k in range(1, 8)] + [dp_peer(k)[1] for k in range(1, 16)]
    barrier = pltpu.get_barrier_semaphore()
    for device in peers:
        pl.semaphore_signal(barrier, inc=1, device_id=device, device_id_type=MESH)
    for i in (3, 4, 0, 1, 2, *range(10, 16)):
        loads[i].start()
    bias_one[...] = jnp.broadcast_to(q_bias[...].reshape(1, HEAD_DIM).astype(F32), bias_one.shape)
    pl.semaphore_wait(barrier, len(peers))
    send = Sender(send_sem, recv_sem)

    half_q, half_o = D // 2, HEAD_DIM // 2

    def q_piece(index, sub=None):
        size = half_q if sub is None else half_q // 2
        start = c * half_q + (0 if sub is None else sub * size)
        return q_all.at[pl.ds(pl.multiple_of(start, 128), size), q_cols(index)]

    parity = lax.rem(y, 2)

    def o_rows(index, side, sub):
        size = half_o // 2 if sub is None else half_o // 4
        start = index * HEAD_DIM + c * half_o + side * (half_o // 2)
        start = start + (0 if sub is None else sub * size)
        return o_all.at[pl.ds(pl.multiple_of(start, 16), size)]

    def o_piece(index, sub=None):
        return o_rows(index, parity, sub)

    def o_other(index, sub):
        return o_rows(index, 1 - parity, sub)

    own_q, own_o = q_piece(t), o_piece(t)
    loads[3].wait()
    loads[4].wait()

    o_u, o_d = send(own_o, o_piece(t), up), send(own_o, o_piece(t), down)
    q_x = send(own_q, q_piece(t), partner)
    q_u, q_d = send(own_q, q_piece(t), up), send(own_q, q_piece(t), down)
    bias_copies = [send(bias_one, bias_all.at[t], tensor_peer(k)) for k in range(1, 8)]
    o_x = send(own_o, o_piece(t), partner)
    for load in loads[5:10]:
        load.start()

    loads[0].wait()
    for load in loads[10:]:
        load.wait()
    x = x_v[...].reshape(2 * SEQ, D)
    normed[...] = rms_rows(x.astype(F32), gain[...].reshape(1, D)).astype(BF16)
    loads[1].wait()
    loads[2].wait()
    cos_rows = jnp.concatenate([cosine[...]] * 2, axis=0)
    sin_rows = jnp.concatenate([sine[...]] * 2, axis=0)
    k_f = jnp.dot(normed[...], k_v[...], preferred_element_type=F32)
    for g in range(KV_HEADS):
        cols = slice(g * HEAD_DIM, (g + 1) * HEAD_DIM)
        keys[:, cols] = rotate(k_f[:, cols], cos_rows, sin_rows).astype(BF16)
    v_f = jnp.dot(normed[...], v_v[...], preferred_element_type=F32)
    values[...] = (v_f + v_bias[...].reshape(1, -1).astype(F32)).astype(BF16)

    q_sib, o_sib = [], []

    def project_q(i):
        cols = pl.ds(pl.multiple_of(i * 256, 256), 256)
        q_f = jnp.dot(normed[...], q_all[:, cols], preferred_element_type=F32)
        for e in range(2):
            q_e = q_f[:, e * HEAD_DIM : (e + 1) * HEAD_DIM] + bias_all[2 * i + e][0:1]
            at = pl.ds(pl.multiple_of(i * 256 + e * HEAD_DIM, HEAD_DIM), HEAD_DIM)
            queries[:, at] = rotate(q_e, cos_rows, sin_rows).astype(BF16)

    def share(piece, index, sub, copies):
        copies.append(send(piece(index, sub), piece(index, sub), sibling))

    def pass_piece(piece, index, sub, device):
        return send(piece(index, sub), piece(index, sub), device)

    y_ahead = {"y": lax.rem(y + 1, 4)}
    y_back = {"y": lax.rem(y + 3, 4)}
    over_y = []

    def spread(index, sub=None):
        share(o_piece, index, sub, o_sib)
        for part, device in ((0, y_ahead), (1, y_back)):
            if sub is None or sub == part:
                piece = o_piece(index, part)
                over_y.append((send(piece, piece, device), index, part))

    def collect(count):
        for _ in range(count):
            copy, index, part = over_y.pop(0)
            copy.wait_recv()
            share(o_other, index, part, o_sib)

    o_u.wait_recv()
    o_fu = pass_piece(o_piece, low, 0, up)
    o_xl = pass_piece(o_piece, low, None, partner)
    spread(low)
    o_d.wait_recv()
    o_fd = pass_piece(o_piece, high, 1, down)
    o_xh = pass_piece(o_piece, high, None, partner)
    spread(high)
    q_x.wait_recv()
    q_xu = pass_piece(q_piece, there, None, up)
    q_xd = pass_piece(q_piece, there, None, down)
    share(q_piece, there, None, q_sib)
    q_u.wait_recv()
    q_fu = pass_piece(q_piece, low, 0, up)
    share(q_piece, low, None, q_sib)
    q_d.wait_recv()
    q_fd = pass_piece(q_piece, high, 1, down)
    share(q_piece, high, None, q_sib)
    collect(4)
    o_x.wait_recv()
    spread(there)
    o_fu.wait_recv()
    o_xfa = pass_piece(o_piece, far, 0, partner)
    spread(far, 0)
    o_fd.wait_recv()
    o_xfb = pass_piece(o_piece, far, 1, partner)
    spread(far, 1)
    for copy in bias_copies:
        copy.wait_recv()
    bias_all[t] = bias_one[...]
    q_sib[0].wait_recv()
    project_q(z)
    o_xl.wait_recv()
    spread(low_x)
    collect(4)
    q_xu.wait_recv()
    q_fxu = pass_piece(q_piece, low_x, 0, up)
    share(q_piece, low_x, None, q_sib)
    q_xd.wait_recv()
    q_fxd = pass_piece(q_piece, high_x, 1, down)
    share(q_piece, high_x, None, q_sib)
    o_xh.wait_recv()
    spread(high_x)
    collect(2)
    q_fu.wait_recv()
    share(q_piece, far, 0, q_sib)
    q_fd.wait_recv()
    share(q_piece, far, 1, q_sib)
    for copy in q_sib[1:5]:
        copy.wait_recv()
    project_q(zm)
    project_q(zp)
    o_xfa.wait_recv()
    spread(far_x, 0)
    o_xfb.wait_recv()
    spread(far_x, 1)
    collect(2)
    q_fxu.wait_recv()
    share(q_piece, far_x, 0, q_sib)
    q_fxd.wait_recv()
    share(q_piece, far_x, 1, q_sib)
    collect(2)
    for copy in q_sib[5:]:
        copy.wait_recv()
    project_q(z2)

    q_pos = lax.broadcasted_iota(jnp.int32, (SEQ, SEQ), 0)
    k_pos = lax.broadcasted_iota(jnp.int32, (SEQ, SEQ), 1)
    group = HEADS // KV_HEADS
    first_pair = (b * 8 + t) * 2
    for copy in o_sib:
        copy.wait_recv()

    def attend(p):
        rows = slice(p * SEQ, (p + 1) * SEQ)
        allowed = (k_pos <= q_pos) & (k_pos < lengths[first_pair + p])
        allowed = jnp.concatenate([allowed.astype(F32)] * group, axis=0) > 0.5
        for g in range(KV_HEADS):
            cols = slice(g * HEAD_DIM, (g + 1) * HEAD_DIM)
            q_g = jnp.concatenate(
                [
                    queries[rows, (g * group + h) * HEAD_DIM : (g * group + h + 1) * HEAD_DIM]
                    for h in range(group)
                ],
                axis=0,
            )
            logits = lax.dot_general(
                q_g, keys[rows, cols], (((1,), (1,)), ((), ())), preferred_element_type=F32
            ) / math.sqrt(HEAD_DIM)
            logits = jnp.where(allowed, logits, -1e30)
            shifted = jnp.exp(logits - jnp.max(logits, axis=-1, keepdims=True))
            probs = (shifted / jnp.sum(shifted, axis=-1, keepdims=True)).astype(BF16)
            ctx = jnp.dot(probs, values[rows, cols], preferred_element_type=F32).astype(BF16)
            for h in range(group):
                at = (g * group + h) * HEAD_DIM
                context[rows, at : at + HEAD_DIM] = ctx[h * SEQ : (h + 1) * SEQ]
        for i in range(D // 256):
            cols = slice(i * 256, (i + 1) * 256)
            attended = jnp.dot(context[rows], o_all[:, cols], preferred_element_type=F32)
            after_v[rows, cols] = (x_v[p, :, cols].astype(F32) + attended).astype(BF16)
        after_rows = after_v[rows].astype(F32)
        gathered[t, rows] = rms_rows(after_rows, mlp_gain[...].reshape(1, D)).astype(BF16)

    def block_rows(g, span):
        return gathered.at[g, pl.ds(span[0], span[1] - span[0])]

    def pass_on(g, span, device):
        return send(block_rows(g, span), block_rows(g, span), device)

    attend(1)
    u2 = pass_on(here, C2, up)
    d2 = pass_on(here, C2, down)
    x2 = pass_on(here, C2, partner)
    attend(0)
    u1 = pass_on(here, C1, up)
    d1 = pass_on(here, C1, down)
    x1 = pass_on(here, C1, partner)

    for load in loads[5:10]:
        load.wait()
    wd[FFL:FFP] = jnp.zeros((FFP - FFL, D), BF16)
    w_tail[TAIL:128] = jnp.zeros((128 - TAIL, D), BF16)
    w_tail[128 + TAIL :] = jnp.zeros((128 - TAIL, D), BF16)

    def gated(gate_values, up_values):
        return (gate_values / (1.0 + jnp.exp(-gate_values)) * up_values).astype(BF16)

    def by_rows(g, weights):
        return lax.dot_general(
            gathered[g], weights, (((1,), (1,)), ((), ())), preferred_element_type=F32
        )

    def block(g, own=False, between=None):
        def hidden(i, carry):
            at = pl.ds(pl.multiple_of(i * 256, 256), 256)
            active[:, at] = gated(by_rows(g, wg[at]), by_rows(g, wu[at]))
            return carry

        lax.fori_loop(0, FULL // 256, hidden, 0, unroll=True)
        both = by_rows(g, w_tail[...])
        active[:, FULL:FFP] = gated(both[:, :128], both[:, 128:])

        for i in range(D // 256):
            if i == D // 512 and between is not None:
                between()
            cols = slice(i * 256, (i + 1) * 256)
            result = jnp.dot(active[...], wd[:, cols], preferred_element_type=F32)
            if own:
                result = result.astype(BF16).astype(F32) + after_v[:, cols].astype(F32)
            result = result.astype(BF16).reshape(2, 8, 16, 256)
            for owner in range(8):
                partial[owner, pl.ds(2 * g, 2), :, cols] = result[:, owner]

    block(here, own=True)

    def tabulate(i, carry):
        query_rows[pl.ds(i, 1)] = jnp.full((1, 128), query_of[i], jnp.int32)
        target_rows[pl.ds(i, 1)] = jnp.full((1, 128), destination[i], jnp.int32)
        return carry

    lax.fori_loop(0, 256, tabulate, 0, unroll=8)
    u2.wait_recv()
    f2u = pass_on(low, C2A, up)
    x_low = pass_on(low, C2, partner)
    d2.wait_recv()
    f2d = pass_on(high, C2B, down)
    x_high = pass_on(high, C2, partner)
    x1.wait_recv()
    xu = pass_on(there, C1, up)
    xd = pass_on(there, C1, down)
    u1.wait_recv()
    f1u = pass_on(low, C1A, up)
    d1.wait_recv()
    f1d = pass_on(high, C1B, down)
    block(low)
    f2u.wait_recv()
    x_far_a = pass_on(far, C2A, partner)
    f2d.wait_recv()
    x_far_b = pass_on(far, C2B, partner)
    block(high)
    x2.wait_recv()
    block(there)
    xu.wait_recv()
    fxu = pass_on(low_x, C1A, up)
    xd.wait_recv()
    fxd = pass_on(high_x, C1B, down)
    x_low.wait_recv()
    block(low_x)
    x_high.wait_recv()
    block(high_x)
    f1u.wait_recv()
    f1d.wait_recv()
    block(far)
    fxu.wait_recv()
    fxd.wait_recv()
    x_far_a.wait_recv()
    x_far_b.wait_recv()

    def add_both(cols, zz, lo, extra):
        def step(i, carry):
            for e in range(2):
                at = (2 * zz + e, lo + i, slice(None), cols)
                partial[at] = (
                    partial[at].astype(F32) + extra[e, i, :, cols].astype(F32)
                ).astype(BF16)
            return carry

        lax.fori_loop(0, extra.shape[1], step, 0, unroll=True)

    def add_one(cols, index, lo, extra):
        def step(i, carry):
            at = (index, lo + i, slice(None), cols)
            partial[at] = (partial[at].astype(F32) + extra[i, :, cols].astype(F32)).astype(BF16)
            return carry

        lax.fori_loop(0, extra.shape[0], step, 0, unroll=True)

    class Half:
        def __init__(self, h):
            self.h, self.sx, self.copies = h, [None] * 4, []
            self.cols = slice(h * (D // 2), (h + 1) * (D // 2))

        def both_of(self, zz, lo, hi):
            return partial.at[pl.ds(2 * zz, 2), pl.ds(lo, hi - lo), :, self.cols]

        def one_of(self, index, lo, hi):
            return partial.at[index, pl.ds(lo, hi - lo), :, self.cols]

        def begin(self):
            cols = self.cols
            self.a_up = send(self.both_of(z2, 0, N1A), r1_low.at[:, :, :, cols], up)
            self.a_down = send(self.both_of(z2, N1A, N1), r1_high.at[:, :, :, cols], down)

        def cross(self, k):
            zz = (z2, zp, zm, z)[k]
            self.sx[k] = send(
                self.one_of(zz * 2 + 1 - xh, N1, 16), r2_x.at[k, :, :, self.cols], partner
            )

        def mid_up(self):
            self.a_up.wait_recv()
            add_both(self.cols, zp, 0, r1_low)
            self.b_up = send(self.both_of(zp, 0, N1), r1_up.at[:, :, :, self.cols], up)

        def mid_down(self):
            self.a_down.wait_recv()
            add_both(self.cols, zm, N1A, r1_high)
            self.b_down = send(self.both_of(zm, 0, N1), r1_down.at[:, :, :, self.cols], down)

        def crossed(self, k):
            self.sx[k].wait_recv()
            add_one(self.cols, (far, high, low, t)[k], N1, r2_x.at[k])
            if k == 0:
                cols = self.cols
                self.c_up = send(self.one_of(far, N1, N2A), r2_low.at[:, :, cols], up)
                self.c_down = send(self.one_of(far, N2A, 16), r2_high.at[:, :, cols], down)

        def third_up(self):
            self.c_up.wait_recv()
            add_one(self.cols, high, N1, r2_low)
            self.e_up = send(self.one_of(high, N1, 16), r2_up.at[:, :, self.cols], up)

        def third_down(self):
            self.c_down.wait_recv()
            add_one(self.cols, low, N2A, r2_high)
            self.e_down = send(self.one_of(low, N1, 16), r2_down.at[:, :, self.cols], down)

        def fold(self):
            cols = self.cols
            self.b_up.wait_recv()
            self.b_down.wait_recv()

            def step(i, carry):
                at = (there, i, slice(None), cols)
                total = partial[at].astype(F32) + r1_up[1 - xh, i, :, cols].astype(F32)
                partial[at] = (total + r1_down[1 - xh, i, :, cols].astype(F32)).astype(BF16)
                return carry

            lax.fori_loop(0, N1, step, 0, unroll=3)
            self.ex = send(self.one_of(there, 0, N1), r1_x.at[:, :, cols], partner)

        def finish_two(self):
            cols = self.cols
            self.e_up.wait_recv()
            self.e_down.wait_recv()

            def step(i, carry):
                at = (t, N1 + i, slice(None), cols)
                total = partial[at].astype(F32) + r2_up[i, :, cols].astype(F32)
                partial[at] = (total + r2_down[i, :, cols].astype(F32)).astype(BF16)
                return carry

            lax.fori_loop(0, 16 - N1, step, 0, unroll=True)

        def finish_one(self):
            cols = self.cols
            self.ex.wait_recv()

            def step(i, carry):
                at = (t, i, slice(None), cols)
                total = partial[at].astype(F32) + r1_up[xh, i, :, cols].astype(F32)
                total = total + r1_down[xh, i, :, cols].astype(F32)
                partial[at] = (total + r1_x[i, :, cols].astype(F32)).astype(BF16)
                return carry

            lax.fori_loop(0, N1, step, 0, unroll=3)

        def relay(self):
            cols = self.cols
            for k in range(16):
                device = dp_peer(k)[1]
                if k == 0:
                    landed[b, :, cols] = partial[t, chosen[k], :, cols]
                else:
                    staged[k, :, cols] = partial[t, chosen[k], :, cols]
                    self.copies.append(
                        send(staged.at[k, :, cols], landed.at[b, :, cols], device)
                    )

        def score(self):
            cols = self.cols
            weight = (final_gain[...] * score_weight[...]).reshape(1, D)[:, cols]
            position = lax.broadcasted_iota(jnp.int32, (16, D // 2), 0)
            for p in range(16):
                wanted = lengths[b * 16 + p] - 1 - t * 16
                row = jnp.where(position == wanted, partial[t, p, :, cols].astype(F32), 0.0)
                last_rows[p : p + 1] = jnp.sum(row, axis=0, keepdims=True)
            found = last_rows[...]
            sums = jnp.sum(found * found, axis=-1, keepdims=True)
            squares[self.h] = jnp.broadcast_to(sums, (16, 128))
            sums = jnp.sum(found * weight, axis=-1, keepdims=True)
            dots[self.h] = jnp.broadcast_to(sums, (16, 128))

    chosen = []
    for k in range(16):
        index = dp_peer(k)[0]
        pair = jnp.int32(0)
        for j in range(1, 16):
            pair = jnp.where(destination[b * 16 + j] == index, j, pair)
        chosen.append(pair)

    halves = (Half(0), Half(1))
    steps = {
        "b": Half.begin,
        "mu": Half.mid_up,
        "md": Half.mid_down,
        "tu": Half.third_up,
        "td": Half.third_down,
        "fo": Half.fold,
        "f2": Half.finish_two,
        "f1": Half.finish_one,
        "re": Half.relay,
        "sc": Half.score,
    }
    for k in range(4):
        steps[f"x{k}"] = functools.partial(Half.cross, k=k)
        steps[f"s{k}"] = functools.partial(Half.crossed, k=k)
    def begin_first():
        for name, h in ORDER[:EARLY]:
            steps[name](halves[h])

    block(far_x, between=begin_first)
    for name, h in ORDER[EARLY:]:
        steps[name](halves[h])

    mean = (squares[0] + squares[1]) / D
    score_one[...] = (dots[0] + dots[1]) * lax.rsqrt(mean + norm_eps)
    copies = [send(score_one, score_eight.at[t], tensor_peer(k)) for k in range(1, 8)]
    score_eight[t] = score_one[...]
    halves[1].relay()
    for copy in copies:
        copy.wait_recv()
    total = score_eight[0]
    for k in range(1, 8):
        total = total + score_eight[k]
    score_sum[...] = total
    score_all[b] = total
    copies = [send(score_sum, score_all.at[b], dp_peer(k)[1]) for k in range(1, 16)]
    writes = []

    def write(src, dst):
        copy = pltpu.make_async_copy(src, dst, local_sem.at[len(loads) + len(writes)])
        copy.start()
        writes.append(copy)

    def write_half(half):
        for copy in half.copies:
            copy.wait_recv()
        write(landed.at[:, :, half.cols], relaid_out.at[:, :, half.cols])

    write_half(halves[0])
    for copy in copies:
        copy.wait_recv()
    pair_scores = score_all[...].reshape(256, 128)
    lane = lax.broadcasted_iota(jnp.int32, (256, 128), 1)
    member = query_rows[...] == lane
    means = jnp.sum(jnp.where(member, pair_scores, 0.0), axis=0, keepdims=True) / PER_QUERY
    own_means = jnp.sum(jnp.where(member, means, 0.0), axis=1, keepdims=True)
    mine = jnp.where(target_rows[...] == b, pair_scores - own_means, 0.0)
    mine = jnp.sum(mine.reshape(16, 16, 128), axis=1)
    at_row = lax.broadcasted_iota(jnp.int32, (16, 128), 0)
    at_lane = lax.broadcasted_iota(jnp.int32, (16, 128), 1)
    centred = jnp.sum(jnp.where(at_row == at_lane, mine, 0.0), axis=0, keepdims=True)
    centred_out[...] = centred.reshape(128)[:16]
    lane = lax.broadcasted_iota(jnp.int32, (1, 128), 1)
    own = jnp.zeros((1, 128), F32)
    for k in range(QUERY_DP):
        mean = jnp.sum(
            jnp.where(lane == b * QUERY_DP + k, means, 0.0), axis=1, keepdims=True
        )
        own = jnp.where(lane == k, mean, own)
    mean_out[...] = own.reshape(128)[:QUERY_DP]
    write_half(halves[1])
    send.drain()
    for copy in writes:
        copy.wait()


def any_spec():
    return pl.BlockSpec(memory_space=pl.ANY)


def vmem_spec():
    return pl.BlockSpec(memory_space=pltpu.VMEM)


def smem_spec():
    return pl.BlockSpec(memory_space=pltpu.SMEM)


def rotary_tables():
    index = np.arange(HEAD_DIM // 2, dtype=np.float32)
    frequency = np.power(np.float64(theta_base), -2.0 * index / HEAD_DIM).astype(np.float32)
    angles = np.arange(SEQ, dtype=np.float32)[:, None] * frequency[None, :]
    cosine, sine = np.cos(angles.astype(np.float64)), np.sin(angles.astype(np.float64))
    return (
        np.concatenate([cosine, cosine], axis=1).astype(np.float32),
        np.concatenate([-sine, sine], axis=1).astype(np.float32),
    )


def on_device(
    arrived, destination, query_of, lengths, attn_gain, q_weight, q_bias, k_weight, v_weight,
    v_bias, o_weight, mlp_gain, w_gate, w_up, w_down, final_gain, score_weight,
):
    cosine, sine = rotary_tables()
    pairs = lambda *lead: pltpu.VMEM((*lead, 16, D), BF16)
    relaid, centred, query_mean = pl.pallas_call(
        layer_kernel,
        out_shape=[
            jax.ShapeDtypeStruct((16, 16, D), BF16),
            jax.ShapeDtypeStruct((16,), F32),
            jax.ShapeDtypeStruct((QUERY_DP,), F32),
        ],
        in_specs=[smem_spec()] * 3 + [vmem_spec()] * 2 + [any_spec()] * 14,
        out_specs=[any_spec()] + [vmem_spec()] * 2,
        scratch_shapes=[
            pltpu.VMEM((D,), F32),
            pltpu.VMEM((D,), F32),
            pltpu.VMEM((D,), F32),
            pltpu.VMEM((D,), F32),
            pltpu.VMEM((SEQ, HEAD_DIM), F32),
            pltpu.VMEM((SEQ, HEAD_DIM), F32),
            pltpu.VMEM((2, SEQ, D), BF16),
            pltpu.VMEM((D, KV_HEADS * HEAD_DIM), BF16),
            pltpu.VMEM((D, KV_HEADS * HEAD_DIM), BF16),
            pltpu.VMEM((D, HEADS * HEAD_DIM), BF16),
            pltpu.VMEM((HEADS * HEAD_DIM, D), BF16),
            pltpu.VMEM((8, HEAD_DIM), F32),
            pltpu.VMEM((8, 8, HEAD_DIM), F32),
            pltpu.VMEM((2 * SEQ, D), BF16),
            pltpu.VMEM((2 * SEQ, KV_HEADS * HEAD_DIM), BF16),
            pltpu.VMEM((2 * SEQ, KV_HEADS * HEAD_DIM), BF16),
            pltpu.VMEM((2 * SEQ, HEADS * HEAD_DIM), BF16),
            pltpu.VMEM((2 * SEQ, HEADS * HEAD_DIM), BF16),
            pltpu.VMEM((2 * SEQ, D), BF16),
            pltpu.VMEM((8, 2 * SEQ, D), BF16),
            pltpu.VMEM((FFL, D), BF16),
            pltpu.VMEM((FFL, D), BF16),
            pltpu.VMEM((FFP, D), BF16),
            pltpu.VMEM((256, D), BF16),
            pltpu.VMEM((2 * SEQ, FFP), BF16),
            pairs(8, 16),
            pairs(2, N1A),
            pairs(2, N1 - N1A),
            pairs(2, N1),
            pairs(2, N1),
            pairs(N1),
            pairs(4, 16 - N1),
            pairs(N2A - N1),
            pairs(16 - N2A),
            pairs(16 - N1),
            pairs(16 - N1),
            pairs(16),
            pairs(16),
            pltpu.VMEM((16, D // 2), F32),
            pltpu.VMEM((2, 16, 128), F32),
            pltpu.VMEM((2, 16, 128), F32),
            pltpu.VMEM((16, 128), F32),
            pltpu.VMEM((8, 16, 128), F32),
            pltpu.VMEM((16, 128), F32),
            pltpu.VMEM((16, 16, 128), F32),
            pltpu.VMEM((256, 128), jnp.int32),
            pltpu.VMEM((256, 128), jnp.int32),
            pltpu.SemaphoreType.DMA((19,)),
            pltpu.SemaphoreType.DMA((176,)),
            pltpu.SemaphoreType.DMA((176,)),
        ],
        compiler_params=pltpu.CompilerParams(
            collective_id=0, has_side_effects=True, vmem_limit_bytes=60 * 2**20
        ),
    )(
        lengths, destination, query_of, q_bias, v_bias, attn_gain, mlp_gain, final_gain, score_weight,
        cosine, sine, arrived, q_weight, k_weight, v_weight, o_weight, w_gate.T, w_up.T, w_down,
    )
    hidden_out = jnp.transpose(relaid, (1, 0, 2))

    return (hidden_out, centred, query_mean)


def solution(mesh):
    split = Mesh(mesh.devices.reshape(4, 2, 2, 4, 2), AXES)
    placed = (
        P(DP + TENSOR, None, None),
        P(),
        P(),
        P(),
        P(),
        P(None, TENSOR),
        P(TENSOR),
        P(),
        P(),
        P(),
        P(TENSOR, None),
        P(),
        P(None, TENSOR),
        P(None, TENSOR),
        P(TENSOR, None),
        P(),
        P(),
    )
    return jax.shard_map(
        on_device,
        mesh=split,
        in_specs=placed,
        out_specs=(P(TENSOR, DP, None), P(DP), P(DP)),
        check_vma=False,
    )
```
